256 devices in a mesh: tm: 8 (over x, y_lo), space: 32 (over y_hi, z, core).
Axes of the slice: x: 4, y: 4 (y_hi: 2, y_lo: 2; y = y_hi * 2 + y_lo), z: 8, core: 2. Of those that a mesh axis runs over, the one named last changes fastest.
Arguments:
- state: float32 [8, 6, 8, 512, 128], P('tm', None, None, 'space'), may hold values from -6 to 6
- multiplier: float32 [8, 6, 8, 512, 128], P('tm', None, None, 'space'), may hold values from -6 to 6
- members: bfloat16 [8, 40, 6, 8, 512, 128], P('tm', None, None, None, 'space'), may hold values from -6 to 6
- static_var: float32 [8, 6, 8, 512, 128], P('tm', None, None, 'space'), may hold values from 0.1 to 1
- courant: float32 [8, 2, 8, 512, 128], P('tm', None, None, 'space'), may hold values from -0.45 to 0.45
- coupling: float32 [8, 6, 6], replicated, may hold values from -2 to 2
- loc_offsets: int32 [9], replicated, may hold values from -8 to 8, as said below
Outputs:
- first_row: float32 [8, 6, 8, 512, 128], P('tm', None, None, 'space')
The draws below stay inside these ranges and needn't reach their ends.
Inputs may be any that keep to these rules, and one draw needn't show every extreme that they name: `loc_offsets`: both -8 and 8 occur among the offsets.
All inputs are finite; a program needn't handle non-finite values.
Results may differ from the reference program's by a relative error of at most 0.0013.
Values may be sent and summed in bfloat16 or wider, within the bound.
A program may use at most 128 MiB of HBM per device.

```python
import math
import jax
import jax.numpy as jnp
from jax import lax

NV = 6
LEV = 8
MEMBERS = 40
TY = 128
NOFF = 9
RMAX = 8
SUBWIN = 8
NX = 512


def draw_loc_offsets(key, part):
    inner = jax.random.randint(key, (NOFF - 2,), -RMAX, RMAX + 1, dtype=jnp.int32)
    ends = jnp.array([-RMAX, RMAX], jnp.int32)
    joined = jnp.concatenate([ends, inner])
    order = jax.random.permutation(jax.random.fold_in(key, 7), NOFF)
    return joined[order]


def shard_levels(key, shape, split, smallest, top_value):
    level = 1.0
    for axis_at, shards_of in split:
        draws = jax.random.uniform(jax.random.fold_in(jax.random.fold_in(key, 6), axis_at), (shards_of,), jnp.float32, smallest / len(split), top_value / len(split))
        level = level * jnp.repeat(jnp.exp(draws), shape[axis_at] // shards_of).reshape((-1,) + (1,) * (len(shape) - 1 - axis_at))
    return level


def noise(stream_key, dims, deviation, bound, shards=(), kind=jnp.bfloat16):
    level = shard_levels(stream_key, dims, shards, -0.22, 0.18) if shards else 1.0
    values = jax.random.normal(stream_key, dims, jnp.float32) * deviation * level
    return jnp.minimum(jnp.maximum(values, -bound), bound).astype(kind)


def setup_inputs(seed: int = 0) -> dict:
    key_list = jax.random.split(jax.random.key(seed), 8)
    state = noise(key_list[0], (SUBWIN, NV, LEV, NX, TY), 1.0, 6.0, ((0, 8), (3, 32)), jnp.float32)
    multiplier = noise(key_list[1], (SUBWIN, NV, LEV, NX, TY), 1.0, 6.0, ((0, 8), (3, 32)), jnp.float32)
    members = noise(key_list[2], (SUBWIN, MEMBERS, NV, LEV, NX, TY), 1.0, 6.0, ((0, 8), (4, 32)))
    static_var = jnp.clip(jnp.exp(math.log(1.0) - 2.3025851 * jax.random.uniform(key_list[3], (SUBWIN, NV, LEV, NX, TY), jnp.float32) ** shard_levels(key_list[3], (SUBWIN, NV, LEV, NX, TY), ((0, 8), (3, 32)), -0.2, 0.2)), 0.1, 1.0)
    courant = jnp.clip(jax.random.uniform(key_list[4], (SUBWIN, 2, LEV, NX, TY), jnp.float32, -0.45, 0.45) * shard_levels(key_list[4], (SUBWIN, 2, LEV, NX, TY), ((0, 8), (3, 32)), -0.4, 0.0), -0.45, 0.45)
    coupling = noise(key_list[5], (LEV, NV, NV), 0.15, 2.0, (), jnp.float32)
    loc_offsets = draw_loc_offsets(jax.random.fold_in(key_list[7], 71), 0)
    return dict(state=state, multiplier=multiplier, members=members, static_var=static_var, courant=courant, coupling=coupling, loc_offsets=loc_offsets)


def tangent_step(padded, winds, coupling):
    center = padded[:, :, 1:-1]
    west_cells = padded[:, :, :-2]
    east_cells = padded[:, :, 2:]
    zero_row = jnp.zeros_like(center[..., :1])
    south_cells = jnp.concatenate([zero_row, center[..., :-1]], axis=-1)
    north_cells = jnp.concatenate([center[..., 1:], zero_row], axis=-1)
    courant_x = winds[0]
    courant_y = winds[1]
    advection = jnp.maximum(courant_x, 0.0) * (center - west_cells)
    advection = advection + jnp.minimum(courant_x, 0.0) * (east_cells - center)
    advection = advection + jnp.maximum(courant_y, 0.0) * (center - south_cells)
    advection = advection + jnp.minimum(courant_y, 0.0) * (north_cells - center)
    coupling_term = jnp.einsum("lvw,wlxy->vlxy", coupling, center, precision=lax.Precision.HIGHEST)
    return center - advection + coupling_term


def periodic_step(field, winds, coupling):
    padded = jnp.concatenate([field[:, :, -1:], field, field[:, :, :1]], axis=2)
    return tangent_step(padded, winds, coupling)


def reference(state, multiplier, members, static_var, courant, coupling, loc_offsets):
    weights = jnp.exp(-0.5 * (loc_offsets.astype(jnp.float32) / RMAX) ** 2)
    results = []
    for window in range(SUBWIN):
        lagrange = multiplier[window]
        ensemble = members[window]
        products = (ensemble.astype(jnp.float32) * lagrange[None]).astype(jnp.bfloat16)
        padded = jnp.concatenate([products[:, :, :, -RMAX:], products, products[:, :, :, :RMAX]], axis=3)

        def add_offset(index, total):
            offset_start = (RMAX + loc_offsets[index]).astype(jnp.int32)
            shifted = lax.dynamic_slice_in_dim(padded, offset_start, NX, 3)
            summed = jnp.sum(ensemble.astype(jnp.float32) * shifted.astype(jnp.float32), axis=0)
            return total + weights[index] * summed

        total = lax.fori_loop(0, NOFF, add_offset, jnp.zeros(lagrange.shape, jnp.float32))
        localized = total / (MEMBERS - 1)
        result = 0.5 * static_var[window] * lagrange + 0.5 * localized + state[window]
        if window >= 1:
            propagated = periodic_step(state[window - 1], courant[window], coupling)
            propagated = periodic_step(propagated, courant[window], coupling)
            result = result - propagated
        results.append(result)
    return jnp.stack(results)
```

```python
import functools
import jax
import jax.numpy as jnp
from jax import lax
from jax.experimental import pallas as pl
from jax.experimental.pallas import tpu as pltpu
from jax.sharding import PartitionSpec as P

MESH = pl.DeviceIdType.MESH
GROUP = 10
RADIUS = 8
LEVELS_PER_CHUNK = 2


def column_of(index, width, side):
    own = GROUP * width
    in_halo = index >= own
    halo_index = index - own
    member = jnp.where(in_halo, halo_index >> 3, index >> 4)
    halo_column = (halo_index & 7) + jnp.where(side == 0, -RADIUS, width)
    column = jnp.where(in_halo, halo_column, index & (width - 1))
    return member, column, in_halo


def stencil_matrix(offsets, side, width, rows, row_start):
    size = GROUP * (width + RADIUS)
    shape = (rows, size)
    row = lax.broadcasted_iota(jnp.int32, shape, 0) + row_start
    col = lax.broadcasted_iota(jnp.int32, shape, 1)
    row_member, row_column, row_halo = column_of(row, width, side)
    col_member, col_column, col_halo = column_of(col, width, side)
    distance = col_column - row_column
    count = jnp.zeros(shape, jnp.float32)
    for j in range(offsets.shape[0]):
        count = count + jnp.where(distance == offsets[j], 1.0, 0.0)
    keep = (row_member == col_member) & ~(row_halo & col_halo)
    scaled = distance.astype(jnp.float32) * (1.0 / RADIUS)
    return jnp.where(keep, count * jnp.exp(-0.5 * scaled * scaled), 0.0)


def kernel(
    sizes,
    offsets,
    coupling,
    state_hbm,
    mult_hbm,
    mem_hbm,
    var_hbm,
    wind_hbm,
    out,
    own,
    halo,
    lam,
    lam_halo,
    state,
    prev,
    var,
    wind,
    state_edge,
    state_halo,
    wind_edge,
    wind_halo,
    total,
    base,
    back_out,
    back_in,
    stencil,
    local_sem,
    own_sem,
    mem_send,
    mem_recv,
    back_send,
    back_recv,
    lam_send,
    lam_recv,
    state_send,
    state_recv,
    edge_send,
    edge_recv,
    wind_send,
    wind_recv,
):
    n_tm, n_space = sizes
    members, n_var, n_lev, width, _ = own.shape
    half = n_var // 2
    per_var = n_lev // LEVELS_PER_CHUNK
    chunks = half * per_var
    t = lax.axis_index("tm")
    s = lax.axis_index("space")
    parity = lax.rem(s, 2)
    t_next, t_last = lax.rem(t + 1, n_tm), lax.rem(t + n_tm - 1, n_tm)
    s_next, s_last = lax.rem(s + 1, n_space), lax.rem(s + n_space - 1, n_space)

    barrier = pltpu.get_barrier_semaphore()
    for peer in ((t, s_next), (t, s_last), (t_last, s), (t_last, s_next), (t_last, s_last)):
        pl.semaphore_signal(barrier, inc=1, device_id=peer, device_id_type=MESH)

    load_state = pltpu.make_async_copy(state_hbm.at[0], state, local_sem.at[0])
    load_wind = pltpu.make_async_copy(
        wind_hbm.at[0], wind.at[:, :, pl.ds(8, width)], local_sem.at[1]
    )
    load_lam = pltpu.make_async_copy(mult_hbm.at[0], lam, local_sem.at[2])
    load_var = pltpu.make_async_copy(var_hbm.at[0], var, local_sem.at[3])
    load_state.start()
    load_wind.start()
    load_lam.start()
    load_var.start()

    def load_own(v):
        return pltpu.make_async_copy(mem_hbm.at[0, :, v], own.at[:, v], own_sem.at[v])

    def neighbour(side):
        return lax.rem(s + n_space - 1 + 2 * side, n_space)

    def send(src, dst, send_sem, recv_sem, where):
        return pltpu.make_async_remote_copy(
            src_ref=src,
            dst_ref=dst,
            send_sem=send_sem,
            recv_sem=recv_sem,
            device_id=where,
            device_id_type=MESH,
        )

    def mem_copy(h, k):
        v, level = k // per_var, lax.rem(k, per_var) * LEVELS_PER_CHUNK
        levels = pl.ds(level, LEVELS_PER_CHUNK)
        rows = pl.ds(pl.multiple_of((1 - h) * RADIUS, RADIUS), RADIUS)
        return send(
            mem_hbm.at[0, :, half * h + v, levels, rows],
            halo.at[h, :, v, levels],
            mem_send.at[h, k],
            mem_recv.at[h, k],
            (t, neighbour(1 - h)),
        )

    def lam_copy(h):
        rows = pl.ds((1 - h) * RADIUS, RADIUS)
        return send(
            mult_hbm.at[0, pl.ds(half * h, half), :, rows],
            lam_halo.at[h],
            lam_send.at[h],
            lam_recv.at[h],
            (t, neighbour(1 - h)),
        )

    def back_copy(h, k):
        v, level = k // per_var, lax.rem(k, per_var) * LEVELS_PER_CHUNK
        levels = pl.ds(level, LEVELS_PER_CHUNK)
        return send(
            back_out.at[h, v, levels],
            back_in.at[h, v, levels],
            back_send.at[h, k],
            back_recv.at[h, k],
            (t, neighbour(h)),
        )

    state_copy = send(
        state_hbm.at[0],
        prev.at[:, :, pl.ds(8, width)],
        state_send.at[0],
        state_recv.at[0],
        (t_next, s),
    )

    def edge_copy(h):
        return send(
            state_edge.at[h],
            state_halo.at[h],
            edge_send.at[h],
            edge_recv.at[h],
            (t_next, neighbour(1 - h)),
        )

    def wind_copy(h):
        return send(
            wind_edge.at[h],
            wind_halo.at[h],
            wind_send.at[h],
            wind_recv.at[h],
            (t, neighbour(1 - h)),
        )

    pl.semaphore_wait(barrier, 5)
    for h in range(2):
        lam_copy(h).start()
    for h in range(2):
        mem_copy(h, 0).start()
    state_copy.start()

    def start_members(k, carry):
        for h in range(2):
            mem_copy(h, k).start()
        return carry

    lax.fori_loop(1, chunks // 2, start_members, 0)

    def start_own(v, carry):
        d2d_side = 1 - parity
        load_own(lax.rem(v // 2 + half * lax.rem(d2d_side + lax.rem(v, 2), 2), n_var)).start()
        return carry

    lax.fori_loop(0, n_var, start_own, 0)

    load_state.wait()
    load_wind.wait()
    for c in range(2):
        state_edge[0, c] = state[:, :, width - 2 + c]
        state_edge[1, c] = state[:, :, c]
    wind_edge[0] = wind[:, :, 8 + width - 1]
    wind_edge[1] = wind[:, :, 8]

    size = GROUP * (width + RADIUS)
    block = 48

    def build(step, carry):
        side = step // (size // block)
        row_start = pl.multiple_of(lax.rem(step, size // block) * block, block)
        matrix = stencil_matrix(offsets, side, width, block, row_start)
        high = matrix.astype(jnp.bfloat16)
        stencil[side, 0, pl.ds(row_start, block)] = high
        stencil[side, 1, pl.ds(row_start, block)] = (matrix - high.astype(jnp.float32)).astype(
            jnp.bfloat16
        )
        return carry

    lax.fori_loop(0, 2 * (size // block), build, 0)
    for h in range(2):
        edge_copy(h).start()
        wind_copy(h).start()
    lax.fori_loop(chunks // 2, chunks, start_members, 0)
    load_lam.wait()

    def one_level(side, v, level):
        full_v = half * side + v
        lam_own = lam[full_v, level]
        lam_far = lam_halo[side, v, level]
        own_sum = jnp.zeros((width, 128), jnp.float32)
        far_sum = jnp.zeros((RADIUS, 128), jnp.float32)
        for pair in range(members // (2 * GROUP)):
            fields, products = [], []
            for q in (2 * pair, 2 * pair + 1):
                near = own[pl.ds(q * GROUP, GROUP), full_v, level].astype(jnp.float32)
                far = halo[side, pl.ds(q * GROUP, GROUP), v, level].astype(jnp.float32)
                fields.append((near, far))
                near = (near * lam_own[None]).reshape(GROUP * width, 128)
                far = (far * lam_far[None]).reshape(GROUP * RADIUS, 128)
                products.append(jnp.concatenate([near, far], axis=0).astype(jnp.bfloat16))
            rhs = jnp.concatenate(products, axis=1)
            smooth = jnp.dot(stencil[side, 0], rhs, preferred_element_type=jnp.float32)
            smooth = smooth + jnp.dot(stencil[side, 1], rhs, preferred_element_type=jnp.float32)
            for i, (near, far) in enumerate(fields):
                part = smooth[:, 128 * i : 128 * (i + 1)]
                own_part = part[: GROUP * width].reshape(GROUP, width, 128)
                far_part = part[GROUP * width :].reshape(GROUP, RADIUS, 128)
                own_sum = own_sum + jnp.sum(near * own_part, axis=0)
                far_sum = far_sum + jnp.sum(far * far_part, axis=0)
        total[full_v, level] = own_sum
        back_out[side, v, level] = far_sum

    def step(j, carry):
        k, over_ici = j // 2, lax.rem(j, 2)
        side = lax.rem(parity + 1 - over_ici, 2)
        v, level = k // per_var, lax.rem(k, per_var) * LEVELS_PER_CHUNK

        @pl.when(lax.rem(k, per_var) == 0)
        def _():
            load_own(half * side + v).wait()

        @pl.when(k == 0)
        def _():
            lam_copy_wait(side)

        mem_copy(side, k).wait_recv()

        def each(d, c):
            one_level(side, v, level + d)
            return c

        lax.fori_loop(0, LEVELS_PER_CHUNK, each, 0)
        back_copy(side, k).start()
        return carry

    def lam_copy_wait(h):
        send(
            mult_hbm.at[0, pl.ds(0, half), :, pl.ds(0, RADIUS)],
            lam_halo.at[h],
            lam_send.at[h],
            lam_recv.at[h],
            (t, neighbour(1 - h)),
        ).wait_recv()

    middle = 2 * ((3 * chunks) // 4)
    lax.fori_loop(0, middle, step, 0)

    state_copy.wait_recv()
    for h in range(2):
        edge_copy(h).wait_recv()
        wind_copy(h).wait_recv()
    load_var.wait()
    padded = width + 16
    rows = lax.broadcasted_iota(jnp.int32, (padded, 128), 0)
    lanes = lax.broadcasted_iota(jnp.int32, (padded, 128), 1)
    for c in range(2):
        prev[:, :, 6 + c] = state_halo[0, c]
        prev[:, :, 8 + width + c] = state_halo[1, c]
    wind[:, :, 7] = wind_halo[0]
    wind[:, :, 8 + width] = wind_halo[1]
    first = jnp.where(t == 0, 0.0, 1.0)

    def tangent(level, carry):
        inside = (rows >= 6) & (rows < 8 + width + 2)
        fields = [jnp.where(inside, prev[v, level], 0.0) for v in range(n_var)]
        wind_x = jnp.where(inside, wind[0, level], 0.0)
        wind_y = jnp.where(inside, wind[1, level], 0.0)
        x_up, x_down = jnp.maximum(wind_x, 0.0), jnp.minimum(wind_x, 0.0)
        y_up, y_down = jnp.maximum(wind_y, 0.0), jnp.minimum(wind_y, 0.0)
        for _ in range(2):
            new = []
            for v in range(n_var):
                f = fields[v]
                west = pltpu.roll(f, 1, 0)
                east = pltpu.roll(f, padded - 1, 0)
                south = jnp.where(lanes == 0, 0.0, pltpu.roll(f, 1, 1))
                north = jnp.where(lanes == 127, 0.0, pltpu.roll(f, 127, 1))
                moved = x_up * (f - west) + x_down * (east - f)
                moved = moved + y_up * (f - south) + y_down * (north - f)
                mixed = coupling[v, level, 0] * fields[0]
                for w in range(1, n_var):
                    mixed = mixed + coupling[v, level, w] * fields[w]
                new.append(f - moved + mixed)
            fields = new
        for v in range(n_var):
            propagated = jnp.where(first > 0.5, fields[v][8 : 8 + width], 0.0)
            base[v, level] = (
                0.5 * var[v, level] * lam[v, level] + state[v, level] - propagated
            )
        return carry

    lax.fori_loop(0, n_lev, tangent, 0)
    lax.fori_loop(middle, 2 * chunks, step, 0)

    def drain(k, carry):
        for h in range(2):
            back_copy(h, k).wait_recv()
            back_copy(h, k).wait_send()
            mem_copy(h, k).wait_send()
        return carry

    lax.fori_loop(0, chunks, drain, 0)
    scale = 0.5 / (members - 1)
    for h in range(2):
        for v in range(half):
            full_v = half * h + v
            lo, hi = (0, RADIUS) if h == 1 else (width - RADIUS, width)
            keep_lo, keep_hi = (RADIUS, width) if h == 1 else (0, width - RADIUS)
            out[0, full_v, :, lo:hi] = base[full_v, :, lo:hi] + scale * (
                total[full_v, :, lo:hi] + back_in[h, v]
            )
            out[0, full_v, :, keep_lo:keep_hi] = (
                base[full_v, :, keep_lo:keep_hi] + scale * total[full_v, :, keep_lo:keep_hi]
            )
    state_copy.wait_send()
    for h in range(2):
        lam_copy(h).wait_send()
        edge_copy(h).wait_send()
        wind_copy(h).wait_send()


def per_device(sizes, state, multiplier, members, static_var, courant, coupling, loc_offsets):
    _, n_mem, n_var, n_lev, width, lanes = members.shape
    half = n_var // 2
    chunks = half * (n_lev // LEVELS_PER_CHUNK)
    size = GROUP * (width + RADIUS)
    f32, bf16 = jnp.float32, jnp.bfloat16
    dma = pltpu.SemaphoreType.DMA
    hbm = pl.BlockSpec(memory_space=pl.ANY)
    smem = pl.BlockSpec(memory_space=pltpu.SMEM)
    return pl.pallas_call(
        functools.partial(kernel, sizes),
        out_shape=jax.ShapeDtypeStruct(state.shape, f32),
        in_specs=[smem, smem, hbm, hbm, hbm, hbm, hbm],
        out_specs=pl.BlockSpec(memory_space=pltpu.VMEM),
        scratch_shapes=[
            pltpu.VMEM((n_mem, n_var, n_lev, width, lanes), bf16),
            pltpu.VMEM((2, n_mem, half, n_lev, RADIUS, lanes), bf16),
            pltpu.VMEM((n_var, n_lev, width, lanes), f32),
            pltpu.VMEM((2, half, n_lev, RADIUS, lanes), f32),
            pltpu.VMEM((n_var, n_lev, width, lanes), f32),
            pltpu.VMEM((n_var, n_lev, width + 16, lanes), f32),
            pltpu.VMEM((n_var, n_lev, width, lanes), f32),
            pltpu.VMEM((2, n_lev, width + 16, lanes), f32),
            pltpu.VMEM((2, 2, n_var, n_lev, lanes), f32),
            pltpu.VMEM((2, 2, n_var, n_lev, lanes), f32),
            pltpu.VMEM((2, 2, n_lev, lanes), f32),
            pltpu.VMEM((2, 2, n_lev, lanes), f32),
            pltpu.VMEM((n_var, n_lev, width, lanes), f32),
            pltpu.VMEM((n_var, n_lev, width, lanes), f32),
            pltpu.VMEM((2, half, n_lev, RADIUS, lanes), f32),
            pltpu.VMEM((2, half, n_lev, RADIUS, lanes), f32),
            pltpu.VMEM((2, 2, size, size), bf16),
            dma((4,)),
            dma((n_var,)),
            dma((2, chunks)),
            dma((2, chunks)),
            dma((2, chunks)),
            dma((2, chunks)),
            dma((2,)),
            dma((2,)),
            dma((1,)),
            dma((1,)),
            dma((2,)),
            dma((2,)),
            dma((2,)),
            dma((2,)),
        ],
        compiler_params=pltpu.CompilerParams(
            collective_id=0, has_side_effects=True, vmem_limit_bytes=67043328
        ),
        name="hybrid_row",
    )(loc_offsets, jnp.transpose(coupling, (1, 0, 2)), state, multiplier, members, static_var, courant)


def solution(mesh):
    sizes = (mesh.shape["tm"], mesh.shape["space"])
    return jax.shard_map(
        functools.partial(per_device, sizes),
        mesh=mesh,
        in_specs=(
            P("tm", None, None, "space", None),
            P("tm", None, None, "space", None),
            P("tm", None, None, None, "space", None),
            P("tm", None, None, "space", None),
            P("tm", None, None, "space", None),
            P(),
            P(),
        ),
        out_specs=P("tm", None, None, "space", None),
        check_vma=False,
    )
```

```python
import functools
import jax
import jax.numpy as jnp
from jax import lax
from jax.experimental import pallas as pl
from jax.experimental.pallas import tpu as pltpu
from jax.sharding import PartitionSpec as P

MESH = pl.DeviceIdType.MESH
GROUP = 10
RADIUS = 8
LEVELS_PER_CHUNK = 2


def column_of(index, width, side):
    own = GROUP * width
    in_halo = index >= own
    halo_index = index - own
    member = jnp.where(in_halo, halo_index >> 3, index >> 4)
    halo_column = (halo_index & 7) + jnp.where(side == 0, -RADIUS, width)
    column = jnp.where(in_halo, halo_column, index & (width - 1))
    return member, column, in_halo


def stencil_matrix(offsets, side, width, rows, row_start):
    size = GROUP * (width + RADIUS)
    shape = (rows, size)
    row = lax.broadcasted_iota(jnp.int32, shape, 0) + row_start
    col = lax.broadcasted_iota(jnp.int32, shape, 1)
    row_member, row_column, row_halo = column_of(row, width, side)
    col_member, col_column, col_halo = column_of(col, width, side)
    distance = col_column - row_column
    count = jnp.zeros(shape, jnp.float32)
    for j in range(offsets.shape[0]):
        count = count + jnp.where(distance == offsets[j], 1.0, 0.0)
    keep = (row_member == col_member) & ~(row_halo & col_halo)
    scaled = distance.astype(jnp.float32) * (1.0 / RADIUS)
    return jnp.where(keep, count * jnp.exp(-0.5 * scaled * scaled), 0.0)


def kernel(
    sizes,
    offsets,
    coupling,
    state_hbm,
    mult_hbm,
    mem_hbm,
    var_hbm,
    wind_hbm,
    out,
    own,
    halo,
    lam,
    lam_halo,
    state,
    prev,
    var,
    wind,
    state_edge,
    state_halo,
    wind_edge,
    wind_halo,
    total,
    base,
    back_out,
    back_in,
    stencil,
    relayed,
    local_sem,
    own_sem,
    mem_send,
    mem_recv,
    back_send,
    back_recv,
    lam_send,
    lam_recv,
    state_send,
    state_recv,
    edge_send,
    edge_recv,
    wind_send,
    wind_recv,
    relay_send,
    relay_recv,
):
    n_tm, n_space = sizes
    members, n_var, n_lev, width, _ = own.shape
    half = n_var // 2
    per_var = n_lev // LEVELS_PER_CHUNK
    chunks = half * per_var
    t = lax.axis_index("tm")
    s = lax.axis_index("space")
    parity = lax.rem(s, 2)
    t_next, t_last = lax.rem(t + 1, n_tm), lax.rem(t + n_tm - 1, n_tm)
    s_next, s_last = lax.rem(s + 1, n_space), lax.rem(s + n_space - 1, n_space)

    planes = n_space // 4
    run = (s // (2 * planes)) * (2 * planes)
    z = lax.rem(s // 2, planes)
    outer = (z == 0) | (z == planes - 1)
    relay_of = jnp.where(z == 0, run + 3, run + 2 * (planes - 2))
    is_relay = (s == run + 3) | (s == run + 2 * (planes - 2))
    served = jnp.where(z == 1, run, run + 2 * (planes - 1))

    barrier = pltpu.get_barrier_semaphore()

    def greet(*peer):
        pl.semaphore_signal(barrier, inc=1, device_id=peer, device_id_type=MESH)

    greet(t, s_next)
    greet(t, s_last)
    greet(t_last, s_next)
    greet(t_last, s_last)
    greet(jnp.where(outer, t, t_last), jnp.where(outer, relay_of, s))

    @pl.when(is_relay)
    def _():
        greet(t_last, served)
        greet(t_last, served + 1)

    load_state = pltpu.make_async_copy(state_hbm.at[0], state, local_sem.at[0])
    load_wind = pltpu.make_async_copy(
        wind_hbm.at[0], wind.at[:, :, pl.ds(8, width)], local_sem.at[1]
    )
    load_lam = pltpu.make_async_copy(mult_hbm.at[0], lam, local_sem.at[2])
    load_var = pltpu.make_async_copy(var_hbm.at[0], var, local_sem.at[3])
    load_state.start()
    load_wind.start()
    load_lam.start()
    load_var.start()

    def load_own(v):
        return pltpu.make_async_copy(mem_hbm.at[0, :, v], own.at[:, v], own_sem.at[v])

    def neighbour(side):
        return lax.rem(s + n_space - 1 + 2 * side, n_space)

    def send(src, dst, send_sem, recv_sem, where):
        return pltpu.make_async_remote_copy(
            src_ref=src,
            dst_ref=dst,
            send_sem=send_sem,
            recv_sem=recv_sem,
            device_id=where,
            device_id_type=MESH,
        )

    def mem_copy(h, k):
        v, level = k // per_var, lax.rem(k, per_var) * LEVELS_PER_CHUNK
        levels = pl.ds(level, LEVELS_PER_CHUNK)
        rows = pl.ds(pl.multiple_of((1 - h) * RADIUS, RADIUS), RADIUS)
        return send(
            mem_hbm.at[0, :, half * h + v, levels, rows],
            halo.at[h, :, v, levels],
            mem_send.at[h, k],
            mem_recv.at[h, k],
            (t, neighbour(1 - h)),
        )

    def lam_copy(h):
        rows = pl.ds((1 - h) * RADIUS, RADIUS)
        return send(
            mult_hbm.at[0, pl.ds(half * h, half), :, rows],
            lam_halo.at[h],
            lam_send.at[h],
            lam_recv.at[h],
            (t, neighbour(1 - h)),
        )

    def back_copy(h, k):
        v, level = k // per_var, lax.rem(k, per_var) * LEVELS_PER_CHUNK
        levels = pl.ds(level, LEVELS_PER_CHUNK)
        return send(
            back_out.at[h, v, levels],
            back_in.at[h, v, levels],
            back_send.at[h, k],
            back_recv.at[h, k],
            (t, neighbour(h)),
        )

    state_copy = send(
        state_hbm.at[0],
        prev.at[:, :, pl.ds(8, width)],
        state_send.at[0],
        state_recv.at[0],
        (t_next, s),
    )

    def edge_copy(h):
        return send(
            state_edge.at[h],
            state_halo.at[h],
            edge_send.at[h],
            edge_recv.at[h],
            (t_next, neighbour(1 - h)),
        )

    def wind_copy(h):
        return send(
            wind_edge.at[h],
            wind_halo.at[h],
            wind_send.at[h],
            wind_recv.at[h],
            (t, neighbour(1 - h)),
        )

    pl.semaphore_wait(barrier, jnp.where(is_relay, 7, 5))
    for h in range(2):
        lam_copy(h).start()
    for h in range(2):
        mem_copy(h, 0).start()

    @pl.when(~outer)
    def _():
        state_copy.start()

    def relay_in(c, where):
        return send(
            state_hbm.at[0], relayed.at[c], relay_send.at[c], relay_recv.at[c], (t_next, where)
        )

    def relay_out(c):
        return send(
            relayed.at[c],
            prev.at[:, :, pl.ds(8, width)],
            relay_send.at[2 + c],
            state_recv.at[0],
            (t, served + c),
        )

    def start_members(k, carry):
        for h in range(2):
            mem_copy(h, k).start()
        return carry

    lax.fori_loop(1, chunks // 2, start_members, 0)

    @pl.when(outer)
    def _():
        relay_in(parity, relay_of).start()

    lax.fori_loop(chunks // 2, chunks, start_members, 0)

    def start_own(v, carry):
        d2d_side = 1 - parity
        load_own(lax.rem(v // 2 + half * lax.rem(d2d_side + lax.rem(v, 2), 2), n_var)).start()
        return carry

    lax.fori_loop(0, n_var, start_own, 0)

    load_state.wait()
    load_wind.wait()
    for c in range(2):
        state_edge[0, c] = state[:, :, width - 2 + c]
        state_edge[1, c] = state[:, :, c]
    wind_edge[0] = wind[:, :, 8 + width - 1]
    wind_edge[1] = wind[:, :, 8]

    size = GROUP * (width + RADIUS)
    block = 48

    def build(step, carry):
        side = step // (size // block)
        row_start = pl.multiple_of(lax.rem(step, size // block) * block, block)
        matrix = stencil_matrix(offsets, side, width, block, row_start)
        high = matrix.astype(jnp.bfloat16)
        stencil[side, 0, pl.ds(row_start, block)] = high
        stencil[side, 1, pl.ds(row_start, block)] = (matrix - high.astype(jnp.float32)).astype(
            jnp.bfloat16
        )
        return carry

    lax.fori_loop(0, 2 * (size // block), build, 0)
    for h in range(2):
        edge_copy(h).start()
        wind_copy(h).start()
    load_lam.wait()

    def one_level(side, v, level):
        full_v = half * side + v
        lam_own = lam[full_v, level]
        lam_far = lam_halo[side, v, level]
        own_sum = jnp.zeros((width, 128), jnp.float32)
        far_sum = jnp.zeros((RADIUS, 128), jnp.float32)
        for pair in range(members // (2 * GROUP)):
            fields, products = [], []
            for q in (2 * pair, 2 * pair + 1):
                near = own[pl.ds(q * GROUP, GROUP), full_v, level].astype(jnp.float32)
                far = halo[side, pl.ds(q * GROUP, GROUP), v, level].astype(jnp.float32)
                fields.append((near, far))
                near = (near * lam_own[None]).reshape(GROUP * width, 128)
                far = (far * lam_far[None]).reshape(GROUP * RADIUS, 128)
                products.append(jnp.concatenate([near, far], axis=0).astype(jnp.bfloat16))
            rhs = jnp.concatenate(products, axis=1)
            smooth = jnp.dot(stencil[side, 0], rhs, preferred_element_type=jnp.float32)
            smooth = smooth + jnp.dot(stencil[side, 1], rhs, preferred_element_type=jnp.float32)
            for i, (near, far) in enumerate(fields):
                part = smooth[:, 128 * i : 128 * (i + 1)]
                own_part = part[: GROUP * width].reshape(GROUP, width, 128)
                far_part = part[GROUP * width :].reshape(GROUP, RADIUS, 128)
                own_sum = own_sum + jnp.sum(near * own_part, axis=0)
                far_sum = far_sum + jnp.sum(far * far_part, axis=0)
        total[full_v, level] = own_sum
        back_out[side, v, level] = far_sum

    def step(j, carry):
        k, over_ici = j // 2, lax.rem(j, 2)
        side = lax.rem(parity + 1 - over_ici, 2)
        v, level = k // per_var, lax.rem(k, per_var) * LEVELS_PER_CHUNK

        @pl.when(lax.rem(k, per_var) == 0)
        def _():
            load_own(half * side + v).wait()

        @pl.when(k == 0)
        def _():
            lam_copy_wait(side)

        mem_copy(side, k).wait_recv()

        def each(d, c):
            one_level(side, v, level + d)
            return c

        lax.fori_loop(0, LEVELS_PER_CHUNK, each, 0)
        back_copy(side, k).start()

        for c, at in ((0, chunks // 2), (1, (3 * chunks) // 4)):

            @pl.when(is_relay & (j == 2 * at))
            def _():
                relay_in(c, s).wait_recv()
                relay_out(c).start()

        return carry

    def lam_copy_wait(h):
        send(
            mult_hbm.at[0, pl.ds(0, half), :, pl.ds(0, RADIUS)],
            lam_halo.at[h],
            lam_send.at[h],
            lam_recv.at[h],
            (t, neighbour(1 - h)),
        ).wait_recv()

    lax.fori_loop(0, 2 * chunks, step, 0)

    state_copy.wait_recv()
    for h in range(2):
        edge_copy(h).wait_recv()
        wind_copy(h).wait_recv()
    load_var.wait()
    padded = width + 16
    rows = lax.broadcasted_iota(jnp.int32, (padded, 128), 0)
    lanes = lax.broadcasted_iota(jnp.int32, (padded, 128), 1)
    for c in range(2):
        prev[:, :, 6 + c] = state_halo[0, c]
        prev[:, :, 8 + width + c] = state_halo[1, c]
    wind[:, :, 7] = wind_halo[0]
    wind[:, :, 8 + width] = wind_halo[1]
    first = jnp.where(t == 0, 0.0, 1.0)

    def tangent(level, carry):
        inside = (rows >= 6) & (rows < 8 + width + 2)
        fields = [jnp.where(inside, prev[v, level], 0.0) for v in range(n_var)]
        wind_x = jnp.where(inside, wind[0, level], 0.0)
        wind_y = jnp.where(inside, wind[1, level], 0.0)
        x_up, x_down = jnp.maximum(wind_x, 0.0), jnp.minimum(wind_x, 0.0)
        y_up, y_down = jnp.maximum(wind_y, 0.0), jnp.minimum(wind_y, 0.0)
        for _ in range(2):
            new = []
            for v in range(n_var):
                f = fields[v]
                west = pltpu.roll(f, 1, 0)
                east = pltpu.roll(f, padded - 1, 0)
                south = jnp.where(lanes == 0, 0.0, pltpu.roll(f, 1, 1))
                north = jnp.where(lanes == 127, 0.0, pltpu.roll(f, 127, 1))
                moved = x_up * (f - west) + x_down * (east - f)
                moved = moved + y_up * (f - south) + y_down * (north - f)
                mixed = coupling[v, level, 0] * fields[0]
                for w in range(1, n_var):
                    mixed = mixed + coupling[v, level, w] * fields[w]
                new.append(f - moved + mixed)
            fields = new
        for v in range(n_var):
            propagated = jnp.where(first > 0.5, fields[v][8 : 8 + width], 0.0)
            base[v, level] = (
                0.5 * var[v, level] * lam[v, level] + state[v, level] - propagated
            )
        return carry

    lax.fori_loop(0, n_lev, tangent, 0)

    def drain(k, carry):
        for h in range(2):
            back_copy(h, k).wait_recv()
            back_copy(h, k).wait_send()
            mem_copy(h, k).wait_send()
        return carry

    lax.fori_loop(0, chunks, drain, 0)
    scale = 0.5 / (members - 1)
    for h in range(2):
        for v in range(half):
            full_v = half * h + v
            lo, hi = (0, RADIUS) if h == 1 else (width - RADIUS, width)
            keep_lo, keep_hi = (RADIUS, width) if h == 1 else (0, width - RADIUS)
            out[0, full_v, :, lo:hi] = base[full_v, :, lo:hi] + scale * (
                total[full_v, :, lo:hi] + back_in[h, v]
            )
            out[0, full_v, :, keep_lo:keep_hi] = (
                base[full_v, :, keep_lo:keep_hi] + scale * total[full_v, :, keep_lo:keep_hi]
            )
    @pl.when(~outer)
    def _():
        state_copy.wait_send()

    @pl.when(outer)
    def _():
        relay_in(parity, relay_of).wait_send()

    @pl.when(is_relay)
    def _():
        for c in range(2):
            relay_out(c).wait_send()

    for h in range(2):
        lam_copy(h).wait_send()
        edge_copy(h).wait_send()
        wind_copy(h).wait_send()


def per_device(sizes, state, multiplier, members, static_var, courant, coupling, loc_offsets):
    _, n_mem, n_var, n_lev, width, lanes = members.shape
    half = n_var // 2
    chunks = half * (n_lev // LEVELS_PER_CHUNK)
    size = GROUP * (width + RADIUS)
    f32, bf16 = jnp.float32, jnp.bfloat16
    dma = pltpu.SemaphoreType.DMA
    hbm = pl.BlockSpec(memory_space=pltpu.HBM)
    smem = pl.BlockSpec(memory_space=pltpu.SMEM)
    return pl.pallas_call(
        functools.partial(kernel, sizes),
        out_shape=jax.ShapeDtypeStruct(state.shape, f32),
        in_specs=[smem, smem, hbm, hbm, hbm, hbm, hbm],
        out_specs=pl.BlockSpec(memory_space=pltpu.VMEM),
        scratch_shapes=[
            pltpu.VMEM((n_mem, n_var, n_lev, width, lanes), bf16),
            pltpu.VMEM((2, n_mem, half, n_lev, RADIUS, lanes), bf16),
            pltpu.VMEM((n_var, n_lev, width, lanes), f32),
            pltpu.VMEM((2, half, n_lev, RADIUS, lanes), f32),
            pltpu.VMEM((n_var, n_lev, width, lanes), f32),
            pltpu.VMEM((n_var, n_lev, width + 16, lanes), f32),
            pltpu.VMEM((n_var, n_lev, width, lanes), f32),
            pltpu.VMEM((2, n_lev, width + 16, lanes), f32),
            pltpu.VMEM((2, 2, n_var, n_lev, lanes), f32),
            pltpu.VMEM((2, 2, n_var, n_lev, lanes), f32),
            pltpu.VMEM((2, 2, n_lev, lanes), f32),
            pltpu.VMEM((2, 2, n_lev, lanes), f32),
            pltpu.VMEM((n_var, n_lev, width, lanes), f32),
            pltpu.VMEM((n_var, n_lev, width, lanes), f32),
            pltpu.VMEM((2, half, n_lev, RADIUS, lanes), f32),
            pltpu.VMEM((2, half, n_lev, RADIUS, lanes), f32),
            pltpu.VMEM((2, 2, size, size), bf16),
            pltpu.VMEM((2, n_var, n_lev, width, lanes), f32),
            dma((4,)),
            dma((n_var,)),
            dma((2, chunks)),
            dma((2, chunks)),
            dma((2, chunks)),
            dma((2, chunks)),
            dma((2,)),
            dma((2,)),
            dma((1,)),
            dma((1,)),
            dma((2,)),
            dma((2,)),
            dma((2,)),
            dma((2,)),
            dma((4,)),
            dma((2,)),
        ],
        compiler_params=pltpu.CompilerParams(
            collective_id=0, has_side_effects=True, vmem_limit_bytes=48 * 1024 * 1024
        ),
        name="hybrid_row",
    )(*[pltpu.with_memory_space_constraint(x, pltpu.HBM) for x in (loc_offsets, jnp.transpose(coupling, (1, 0, 2)), state, multiplier, members, static_var, courant)])


def solution(mesh):
    sizes = (mesh.shape["tm"], mesh.shape["space"])
    return jax.shard_map(
        functools.partial(per_device, sizes),
        mesh=mesh,
        in_specs=(
            P("tm", None, None, "space", None),
            P("tm", None, None, "space", None),
            P("tm", None, None, None, "space", None),
            P("tm", None, None, "space", None),
            P("tm", None, None, "space", None),
            P(),
            P(),
        ),
        out_specs=P("tm", None, None, "space", None),
        check_vma=False,
    )
```

```python
import functools
import jax
import jax.numpy as jnp
from jax import lax
from jax.experimental import pallas as pl
from jax.experimental.pallas import tpu as pltpu
from jax.sharding import PartitionSpec as P

MESH = pl.DeviceIdType.MESH
GROUP = 10
DEPTH = 256
LEAD = 4
RADIUS = 8
LEVELS_PER_CHUNK = 2


def column_of(index, width, side):
    own = GROUP * width
    in_halo = index >= own
    halo_index = index - own
    member = jnp.where(in_halo, halo_index >> 3, index >> 4)
    halo_column = (halo_index & 7) + jnp.where(side == 0, -RADIUS, width)
    column = jnp.where(in_halo, halo_column, index & (width - 1))
    return member, column, in_halo


def stencil_matrix(offsets, side, width, rows, row_start):
    shape = (rows, DEPTH)
    row = lax.broadcasted_iota(jnp.int32, shape, 0) + row_start
    col = lax.broadcasted_iota(jnp.int32, shape, 1)
    row_member, row_column, row_halo = column_of(row, width, side)
    col_member, col_column, col_halo = column_of(col, width, side)
    distance = col_column - row_column
    count = jnp.zeros(shape, jnp.float32)
    for j in range(offsets.shape[0]):
        count = count + jnp.where(distance == offsets[j], 1.0, 0.0)
    keep = (row_member == col_member) & ~(row_halo & col_halo)
    scaled = distance.astype(jnp.float32) * (1.0 / RADIUS)
    return jnp.where(keep, count * jnp.exp(-0.5 * scaled * scaled), 0.0)


def kernel(
    sizes,
    offsets_hbm,
    coupling_hbm,
    state_hbm,
    mult_hbm,
    mem_hbm,
    var_hbm,
    wind_hbm,
    out,
    own,
    halo,
    lam,
    lam_halo,
    state,
    prev,
    var,
    wind,
    state_edge,
    state_halo,
    wind_edge,
    wind_halo,
    total,
    base,
    back_out,
    back_in,
    stencil,
    relayed,
    extra,
    extra_lam,
    offsets,
    coupling,
    local_sem,
    own_sem,
    mem_send,
    mem_recv,
    back_send,
    back_recv,
    lam_send,
    lam_recv,
    state_send,
    state_recv,
    edge_send,
    edge_recv,
    wind_send,
    wind_recv,
    relay_send,
    relay_recv,
    extra_send,
    extra_recv,
):
    n_tm, n_space = sizes
    members, n_var, n_lev, width, _ = own.shape
    half, half_lev = n_var // 2, n_lev // 2
    per_var = n_lev // LEVELS_PER_CHUNK
    chunks = half * per_var
    t = lax.axis_index("tm")
    s = lax.axis_index("space")
    parity = lax.rem(s, 2)
    t_next, t_last = lax.rem(t + 1, n_tm), lax.rem(t + n_tm - 1, n_tm)
    s_next, s_last = lax.rem(s + 1, n_space), lax.rem(s + n_space - 1, n_space)

    planes = n_space // 4
    run = (s // (2 * planes)) * (2 * planes)
    z = lax.rem(s // 2, planes)
    outer = (z == 0) | (z == planes - 1)
    relay_of = jnp.where(z == 0, run + 3, run + 2 * (planes - 2))
    wrap = ((z == 0) & (parity == 0)) | ((z == planes - 1) & (parity == 1))
    late = outer & ~wrap
    is_relay = (s == run + 3) | (s == run + 2 * (planes - 2))
    served = jnp.where(z == 1, run, run + 2 * planes - 1)
    served_late = jnp.where(z == 1, run + 1, run + 2 * planes - 2)

    barrier = pltpu.get_barrier_semaphore()

    def greet(*peer):
        pl.semaphore_signal(barrier, inc=1, device_id=peer, device_id_type=MESH)

    greet(t, s_next)
    greet(t, s_last)
    greet(t_last, s_next)
    greet(t_last, s_last)
    greet(jnp.where(wrap, t, t_last), jnp.where(wrap, relay_of, s))

    @pl.when(late)
    def _():
        greet(t, relay_of)

    @pl.when(is_relay)
    def _():
        greet(t_last, served)
        greet(t_last, served_late)

    load_state = pltpu.make_async_copy(state_hbm.at[0], state, local_sem.at[0])
    load_wind = pltpu.make_async_copy(
        wind_hbm.at[0], wind.at[:, :, pl.ds(8, width)], local_sem.at[1]
    )
    load_lam = pltpu.make_async_copy(mult_hbm.at[0], lam, local_sem.at[2])
    load_var = pltpu.make_async_copy(var_hbm.at[0], var, local_sem.at[3])
    def load_own(v):
        return pltpu.make_async_copy(mem_hbm.at[0, :, v], own.at[:, v], own_sem.at[v])

    load_offsets = pltpu.make_async_copy(offsets_hbm, offsets, local_sem.at[4])
    load_coupling = pltpu.make_async_copy(coupling_hbm, coupling, local_sem.at[5])
    load_lam.start()
    for v in range(half):
        load_own(v).start()
        load_own(half + v).start()
        if v == 0:
            load_state.start()
            load_wind.start()
    load_offsets.start()
    load_coupling.start()
    load_var.start()

    def neighbour(side):
        return lax.rem(s + n_space - 1 + 2 * side, n_space)

    def send(src, dst, send_sem, recv_sem, where):
        return pltpu.make_async_remote_copy(
            src_ref=src,
            dst_ref=dst,
            send_sem=send_sem,
            recv_sem=recv_sem,
            device_id=where,
            device_id_type=MESH,
        )

    def mem_copy(h, k):
        v, level = k // per_var, lax.rem(k, per_var) * LEVELS_PER_CHUNK
        levels = pl.ds(level, LEVELS_PER_CHUNK)
        rows = pl.ds(pl.multiple_of((1 - h) * RADIUS, RADIUS), RADIUS)
        return send(
            own.at[:, half * h + v, levels, rows],
            halo.at[h, :, v, levels],
            mem_send.at[h, k],
            mem_recv.at[h, k],
            (t, neighbour(1 - h)),
        )

    def lam_copy(h):
        rows = pl.ds((1 - h) * RADIUS, RADIUS)
        return send(
            lam.at[pl.ds(half * h, half), :, rows],
            lam_halo.at[h],
            lam_send.at[h],
            lam_recv.at[h],
            (t, neighbour(1 - h)),
        )

    def back_copy(h, k):
        v, level = k // per_var, lax.rem(k, per_var) * LEVELS_PER_CHUNK
        levels = pl.ds(level, LEVELS_PER_CHUNK)
        return send(
            back_out.at[h, v, levels],
            back_in.at[h, v, levels],
            back_send.at[h, k],
            back_recv.at[h, k],
            (t, neighbour(h)),
        )

    def part_of(ref, p):
        return ref.at[:, pl.ds(half_lev * p, half_lev)]

    def state_copy(p):
        return send(
            part_of(state_hbm.at[0], p),
            part_of(prev, p).at[:, :, pl.ds(8, width)],
            state_send.at[p],
            state_recv.at[p],
            (t_next, s),
        )

    def relay_in(slot):
        return send(
            part_of(state_hbm.at[0], min(slot, 1)),
            relayed.at[slot],
            relay_send.at[slot],
            relay_recv.at[slot],
            (t_next, relay_of),
        )

    def relay_out(slot):
        return send(
            relayed.at[slot],
            part_of(prev, min(slot, 1)).at[:, :, pl.ds(8, width)],
            relay_send.at[3 + slot],
            state_recv.at[min(slot, 1)],
            (t, served if slot < 2 else served_late),
        )

    last = chunks - 1
    last_levels = pl.ds(n_lev - LEVELS_PER_CHUNK, LEVELS_PER_CHUNK)
    facing = pl.ds(pl.multiple_of(parity * RADIUS, RADIUS), RADIUS)
    extra_copy = send(
        own.at[:, half * parity + half - 1, last_levels, facing],
        extra,
        extra_send.at[0],
        extra_recv.at[0],
        (t, neighbour(parity)),
    )
    extra_lam_copy = send(
        lam.at[half * parity + half - 1, last_levels, facing],
        extra_lam,
        extra_send.at[1],
        extra_recv.at[1],
        (t, neighbour(parity)),
    )

    def edge_copy(h):
        return send(
            state_edge.at[h],
            state_halo.at[h],
            edge_send.at[h],
            edge_recv.at[h],
            (t_next, neighbour(1 - h)),
        )

    def wind_copy(h):
        return send(
            wind_edge.at[h],
            wind_halo.at[h],
            wind_send.at[h],
            wind_recv.at[h],
            (t, neighbour(1 - h)),
        )

    pl.semaphore_wait(barrier, jnp.where(is_relay, 7, jnp.where(late, 6, 5)))
    load_lam.wait()
    for h in range(2):
        lam_copy(h).start()
    load_own(0).wait()
    load_own(half).wait()
    for h in range(2):
        mem_copy(h, 0).start()

    @pl.when(~outer)
    def _():
        state_copy(0).start()
        state_copy(1).start()

    def start_members(k, carry):
        for h in range(2):
            mem_copy(h, k).start()
        return carry

    @pl.when(wrap)
    def _():
        relay_in(0).start()
        relay_in(1).start()
        extra_lam_copy.start()

    lax.fori_loop(1, per_var, start_members, 0)

    @pl.when(late)
    def _():
        relay_in(2).start()

    load_state.wait()
    load_wind.wait()
    for c in range(2):
        state_edge[0, c] = state[:, :, width - 2 + c]
        state_edge[1, c] = state[:, :, c]
    wind_edge[0] = wind[:, :, 8 + width - 1]
    wind_edge[1] = wind[:, :, 8]

    for h in range(2):
        edge_copy(h).start()
        wind_copy(h).start()
    for v in range(1, half):
        load_own(v).wait()
        load_own(half + v).wait()
        lax.fori_loop(per_var * v, per_var * (v + 1), start_members, 0)

    @pl.when(wrap)
    def _():
        extra_copy.start()

    size = GROUP * (width + RADIUS)
    block = 48

    def build(step, carry):
        side = step // (size // block)
        row_start = pl.multiple_of(lax.rem(step, size // block) * block, block)
        matrix = stencil_matrix(offsets, side, width, block, row_start)
        high = matrix.astype(jnp.bfloat16)
        rows = pl.ds(row_start, block)
        stencil[side, rows, :DEPTH] = high
        stencil[side, rows, DEPTH:] = (matrix - high.astype(jnp.float32)).astype(jnp.bfloat16)
        return carry

    load_offsets.wait()
    lax.fori_loop(0, 2 * (size // block), build, 0)
    def sums(side, full_v, level, lam_far, far_fields, near_products):
        lam_own = lam[full_v, level]
        own_sum = jnp.zeros((width, 128), jnp.float32)
        far_sum = jnp.zeros((RADIUS, 128), jnp.float32)
        for pair in range(members // (2 * GROUP)):
            fields, products = [], []
            for q in (2 * pair, 2 * pair + 1):
                near = own[pl.ds(q * GROUP, GROUP), full_v, level].astype(jnp.float32)
                far = far_fields(pl.ds(q * GROUP, GROUP)).astype(jnp.float32)
                fields.append((near, far))
                near = near * lam_own[None] if near_products else jnp.zeros_like(near)
                near = near.reshape(GROUP * width, 128)
                far = (far * lam_far[None]).reshape(GROUP * RADIUS, 128)
                rest = jnp.zeros((DEPTH - GROUP * (width + RADIUS), 128), jnp.float32)
                product = jnp.concatenate([near, far, rest], axis=0).astype(jnp.bfloat16)
                products.append(jnp.concatenate([product, product], axis=0))
            rhs = jnp.concatenate(products, axis=1)
            smooth = jnp.dot(stencil[side], rhs, preferred_element_type=jnp.float32)
            for i, (near, far) in enumerate(fields):
                part = smooth[:, 128 * i : 128 * (i + 1)]
                own_part = part[: GROUP * width].reshape(GROUP, width, 128)
                far_part = part[GROUP * width :].reshape(GROUP, RADIUS, 128)
                own_sum = own_sum + jnp.sum(near * own_part, axis=0)
                far_sum = far_sum + jnp.sum(far * far_part, axis=0)
        return own_sum, far_sum

    def one_level(side, v, level):
        total[half * side + v, level], back_out[side, v, level] = sums(
            side,
            half * side + v,
            level,
            lam_halo[side, v, level],
            lambda group: halo[side, group, v, level],
            True,
        )

    def extra_level(d, carry):
        level = n_lev - LEVELS_PER_CHUNK + d
        own_sum, _ = sums(
            parity,
            half * (1 - parity) + half - 1,
            level,
            extra_lam[d],
            lambda group: extra[group, d],
            False,
        )
        back_in[1 - parity, half - 1, level] = jnp.where(
            parity == 0, own_sum[:RADIUS], own_sum[width - RADIUS :]
        )
        return carry

    def step(j, carry):
        turn = j - LEAD
        in_turn = (turn >= 0) & (j < 2 * chunks - LEAD)
        over_ici = jnp.where(in_turn, 1 - lax.rem(turn + 2 * chunks, 2), jnp.where(turn < 0, 0, 1))
        k = jnp.where(
            in_turn,
            jnp.where(over_ici == 1, turn // 2, LEAD + turn // 2),
            jnp.where(turn < 0, j, j - chunks),
        )
        side = lax.rem(parity + 1 - over_ici, 2)
        v, level = k // per_var, lax.rem(k, per_var) * LEVELS_PER_CHUNK

        @pl.when(k == 0)
        def _():
            lam_copy_wait(side)

        mem_copy(side, k).wait_recv()

        def each(d, c):
            one_level(side, v, level + d)
            return c

        lax.fori_loop(0, LEVELS_PER_CHUNK, each, 0, unroll=True)

        @pl.when(~(wrap & (side == parity) & (k == last)))
        def _():
            back_copy(side, k).start()

        for slot, at in ((0, chunks // 3), (1, chunks // 2), (2, (2 * chunks) // 3)):

            @pl.when(is_relay & (over_ici == 1) & (k == at))
            def _():
                relay_in(slot).wait_recv()
                relay_out(slot).start()

        @pl.when(late & (over_ici == 1) & (k == (2 * chunks) // 3))
        def _():
            state_copy(0).start()

        return carry

    def lam_copy_wait(h):
        send(
            lam.at[pl.ds(0, half), :, pl.ds(0, RADIUS)],
            lam_halo.at[h],
            lam_send.at[h],
            lam_recv.at[h],
            (t, neighbour(1 - h)),
        ).wait_recv()

    lax.fori_loop(0, 2 * chunks, step, 0)

    def drain_sends(k, carry):
        for h in range(2):
            mem_copy(h, k).wait_send()
        return carry

    def drain_back(k, carry):
        for h in range(2):

            @pl.when(~(wrap & (h == 1 - parity) & (k == last)))
            def _():
                back_copy(h, k).wait_recv()

        return carry

    def drain_back_sends(k, carry):
        for h in range(2):

            @pl.when(~(wrap & (h == parity) & (k == last)))
            def _():
                back_copy(h, k).wait_send()

        return carry

    lax.fori_loop(0, chunks, drain_sends, 0)
    load_coupling.wait()

    @pl.when(~wrap)
    def _():
        state_copy(0).wait_send()

    @pl.when(~outer)
    def _():
        state_copy(1).wait_send()

    @pl.when(wrap)
    def _():
        relay_in(0).wait_send()
        relay_in(1).wait_send()
        extra_copy.wait_send()
        extra_lam_copy.wait_send()

    @pl.when(late)
    def _():
        relay_in(2).wait_send()

    @pl.when(is_relay)
    def _():
        for slot in range(3):
            relay_out(slot).wait_send()

    for h in range(2):
        lam_copy(h).wait_send()
        edge_copy(h).wait_send()
        wind_copy(h).wait_send()

    for h in range(2):
        edge_copy(h).wait_recv()
        wind_copy(h).wait_recv()
    load_var.wait()
    padded = width + 16
    rows = lax.broadcasted_iota(jnp.int32, (padded, 128), 0)
    lanes = lax.broadcasted_iota(jnp.int32, (padded, 128), 1)
    wind[:, :, 7] = wind_halo[0]
    wind[:, :, 8 + width] = wind_halo[1]
    first = jnp.where(t == 0, 0.0, 1.0)

    def tangent(level, carry):
        inside = (rows >= 6) & (rows < 8 + width + 2)
        fields = [jnp.where(inside, prev[v, level], 0.0) for v in range(n_var)]
        wind_x = jnp.where(inside, wind[0, level], 0.0)
        wind_y = jnp.where(inside, wind[1, level], 0.0)
        x_up, x_down = jnp.maximum(wind_x, 0.0), jnp.minimum(wind_x, 0.0)
        y_up, y_down = jnp.maximum(wind_y, 0.0), jnp.minimum(wind_y, 0.0)
        for _ in range(2):
            new = []
            for v in range(n_var):
                f = fields[v]
                west = pltpu.roll(f, 1, 0)
                east = pltpu.roll(f, padded - 1, 0)
                south = jnp.where(lanes == 0, 0.0, pltpu.roll(f, 1, 1))
                north = jnp.where(lanes == 127, 0.0, pltpu.roll(f, 127, 1))
                moved = x_up * (f - west) + x_down * (east - f)
                moved = moved + y_up * (f - south) + y_down * (north - f)
                mixed = coupling[v, level, 0] * fields[0]
                for w in range(1, n_var):
                    mixed = mixed + coupling[v, level, w] * fields[w]
                new.append(f - moved + mixed)
            fields = new
        for v in range(n_var):
            propagated = jnp.where(first > 0.5, fields[v][8 : 8 + width], 0.0)
            base[v, level] = (
                0.5 * var[v, level] * lam[v, level] + state[v, level] - propagated
            )
        return carry

    for p in (1, 0):
        state_copy(p).wait_recv()
        levels = pl.ds(half_lev * p, half_lev)
        for c in range(2):
            prev[:, levels, 6 + c] = state_halo[0, c, :, levels]
            prev[:, levels, 8 + width + c] = state_halo[1, c, :, levels]
        lax.fori_loop(half_lev * p, half_lev * (p + 1), tangent, 0)

    @pl.when(wrap)
    def _():
        extra_copy.wait_recv()
        extra_lam_copy.wait_recv()
        lax.fori_loop(0, LEVELS_PER_CHUNK, extra_level, 0)


    scale = 0.5 / (members - 1)

    def compose(v, carry):
        out[0, v] = base[v] + scale * total[v]
        return carry

    lax.fori_loop(0, n_var, compose, 0)
    lax.fori_loop(0, chunks, drain_back_sends, 0)
    lax.fori_loop(0, chunks, drain_back, 0)
    for h in range(2):
        edge = pl.ds(0, RADIUS) if h == 1 else pl.ds(width - RADIUS, RADIUS)
        for v in range(half):
            out[0, half * h + v, :, edge] += scale * back_in[h, v]


def per_device(sizes, state, multiplier, members, static_var, courant, coupling, loc_offsets):
    _, n_mem, n_var, n_lev, width, lanes = members.shape
    half = n_var // 2
    chunks = half * (n_lev // LEVELS_PER_CHUNK)
    size = GROUP * (width + RADIUS)
    f32, bf16 = jnp.float32, jnp.bfloat16
    dma = pltpu.SemaphoreType.DMA
    hbm = pl.BlockSpec(memory_space=pltpu.HBM)
    offsets_shape = loc_offsets.shape
    coupling_shape = (n_var, n_lev, n_var)
    return pl.pallas_call(
        functools.partial(kernel, sizes),
        out_shape=jax.ShapeDtypeStruct(state.shape, f32),
        in_specs=[hbm] * 7,
        out_specs=pl.BlockSpec(memory_space=pltpu.VMEM),
        scratch_shapes=[
            pltpu.VMEM((n_mem, n_var, n_lev, width, lanes), bf16),
            pltpu.VMEM((2, n_mem, half, n_lev, RADIUS, lanes), bf16),
            pltpu.VMEM((n_var, n_lev, width, lanes), f32),
            pltpu.VMEM((2, half, n_lev, RADIUS, lanes), f32),
            pltpu.VMEM((n_var, n_lev, width, lanes), f32),
            pltpu.VMEM((n_var, n_lev, width + 16, lanes), f32),
            pltpu.VMEM((n_var, n_lev, width, lanes), f32),
            pltpu.VMEM((2, n_lev, width + 16, lanes), f32),
            pltpu.VMEM((2, 2, n_var, n_lev, lanes), f32),
            pltpu.VMEM((2, 2, n_var, n_lev, lanes), f32),
            pltpu.VMEM((2, 2, n_lev, lanes), f32),
            pltpu.VMEM((2, 2, n_lev, lanes), f32),
            pltpu.VMEM((n_var, n_lev, width, lanes), f32),
            pltpu.VMEM((n_var, n_lev, width, lanes), f32),
            pltpu.VMEM((2, half, n_lev, RADIUS, lanes), f32),
            pltpu.VMEM((2, half, n_lev, RADIUS, lanes), f32),
            pltpu.VMEM((2, size, 2 * DEPTH), bf16),
            pltpu.VMEM((3, n_var, n_lev // 2, width, lanes), f32),
            pltpu.VMEM((n_mem, LEVELS_PER_CHUNK, RADIUS, lanes), bf16),
            pltpu.VMEM((LEVELS_PER_CHUNK, RADIUS, lanes), f32),
            pltpu.SMEM(offsets_shape, jnp.int32),
            pltpu.SMEM(coupling_shape, f32),
            dma((6,)),
            dma((n_var,)),
            dma((2, chunks)),
            dma((2, chunks)),
            dma((2, chunks)),
            dma((2, chunks)),
            dma((2,)),
            dma((2,)),
            dma((2,)),
            dma((2,)),
            dma((2,)),
            dma((2,)),
            dma((2,)),
            dma((2,)),
            dma((6,)),
            dma((3,)),
            dma((2,)),
            dma((2,)),
        ],
        compiler_params=pltpu.CompilerParams(
            collective_id=0, has_side_effects=True, vmem_limit_bytes=48 * 1024 * 1024
        ),
        name="hybrid_row",
    )(*[pltpu.with_memory_space_constraint(x, pltpu.HBM) for x in (loc_offsets, jnp.transpose(coupling, (1, 0, 2)), state, multiplier, members, static_var, courant)])


def solution(mesh):
    sizes = (mesh.shape["tm"], mesh.shape["space"])
    return jax.shard_map(
        functools.partial(per_device, sizes),
        mesh=mesh,
        in_specs=(
            P("tm", None, None, "space", None),
            P("tm", None, None, "space", None),
            P("tm", None, None, None, "space", None),
            P("tm", None, None, "space", None),
            P("tm", None, None, "space", None),
            P(),
            P(),
        ),
        out_specs=P("tm", None, None, "space", None),
        check_vma=False,
    )
```

```python
import functools
import jax
import jax.numpy as jnp
from jax import lax
from jax.experimental import pallas as pl
from jax.experimental.pallas import tpu as pltpu
from jax.sharding import PartitionSpec as P

MESH = pl.DeviceIdType.MESH
GROUP = 10
DEPTH = 256
LEAD = 4
RADIUS = 8
LEVELS_PER_CHUNK = 2


def column_of(index, width, side):
    own = GROUP * width
    in_halo = index >= own
    halo_index = index - own
    member = jnp.where(in_halo, halo_index >> 3, index >> 4)
    halo_column = (halo_index & 7) + jnp.where(side == 0, -RADIUS, width)
    column = jnp.where(in_halo, halo_column, index & (width - 1))
    return member, column, in_halo


def stencil_matrix(offsets, side, width, rows, row_start):
    shape = (rows, DEPTH)
    row = lax.broadcasted_iota(jnp.int32, shape, 0) + row_start
    col = lax.broadcasted_iota(jnp.int32, shape, 1)
    row_member, row_column, row_halo = column_of(row, width, side)
    col_member, col_column, col_halo = column_of(col, width, side)
    distance = col_column - row_column
    count = jnp.zeros(shape, jnp.float32)
    for j in range(offsets.shape[0]):
        count = count + jnp.where(distance == offsets[j], 1.0, 0.0)
    keep = (row_member == col_member) & ~(row_halo & col_halo)
    scaled = distance.astype(jnp.float32) * (1.0 / RADIUS)
    return jnp.where(keep, count * jnp.exp(-0.5 * scaled * scaled), 0.0)


def kernel(
    sizes,
    offsets_hbm,
    coupling_hbm,
    state_hbm,
    mult_hbm,
    mem_hbm,
    var_hbm,
    wind_hbm,
    out,
    own,
    halo,
    lam,
    lam_halo,
    state,
    prev,
    var,
    wind,
    state_edge,
    state_halo,
    wind_edge,
    wind_halo,
    total,
    base,
    back_out,
    back_in,
    stencil,
    lam_edge,
    extra_lam_edge,
    relayed,
    extra,
    extra_lam,
    offsets,
    coupling,
    local_sem,
    own_sem,
    mem_send,
    mem_recv,
    back_send,
    back_recv,
    lam_send,
    lam_recv,
    state_send,
    state_recv,
    edge_send,
    edge_recv,
    wind_send,
    wind_recv,
    relay_send,
    relay_recv,
    extra_send,
    extra_recv,
):
    n_tm, n_space = sizes
    members, n_var, n_lev, width, _ = own.shape
    half, half_lev = n_var // 2, n_lev // 2
    per_var = n_lev // LEVELS_PER_CHUNK
    chunks = half * per_var
    t = lax.axis_index("tm")
    s = lax.axis_index("space")
    parity = lax.rem(s, 2)
    t_next, t_last = lax.rem(t + 1, n_tm), lax.rem(t + n_tm - 1, n_tm)
    s_next, s_last = lax.rem(s + 1, n_space), lax.rem(s + n_space - 1, n_space)

    planes = n_space // 4
    run = (s // (2 * planes)) * (2 * planes)
    z = lax.rem(s // 2, planes)
    outer = (z == 0) | (z == planes - 1)
    relay_of = jnp.where(z == 0, run + 3, run + 2 * (planes - 2))
    wrap = ((z == 0) & (parity == 0)) | ((z == planes - 1) & (parity == 1))
    late = outer & ~wrap
    is_relay = (s == run + 3) | (s == run + 2 * (planes - 2))
    served = jnp.where(z == 1, run, run + 2 * planes - 1)
    served_late = jnp.where(z == 1, run + 1, run + 2 * planes - 2)

    barrier = pltpu.get_barrier_semaphore()

    def greet(*peer):
        pl.semaphore_signal(barrier, inc=1, device_id=peer, device_id_type=MESH)

    greet(t, s_next)
    greet(t, s_last)
    greet(t_last, s_next)
    greet(t_last, s_last)
    greet(jnp.where(wrap, t, t_last), jnp.where(wrap, relay_of, s))

    @pl.when(late)
    def _():
        greet(t, relay_of)

    @pl.when(is_relay)
    def _():
        greet(t_last, served)
        greet(t_last, served_late)

    load_state = pltpu.make_async_copy(state_hbm.at[0], state, local_sem.at[0])
    load_wind = pltpu.make_async_copy(
        wind_hbm.at[0], wind.at[:, :, pl.ds(8, width)], local_sem.at[1]
    )
    load_lam = pltpu.make_async_copy(mult_hbm.at[0], lam, local_sem.at[2])
    load_var = pltpu.make_async_copy(var_hbm.at[0], var, local_sem.at[3])
    def load_own(v):
        return pltpu.make_async_copy(mem_hbm.at[0, :, v], own.at[:, v], own_sem.at[v])

    load_offsets = pltpu.make_async_copy(offsets_hbm, offsets, local_sem.at[4])
    load_coupling = pltpu.make_async_copy(coupling_hbm, coupling, local_sem.at[5])
    load_lam.start()
    for v in range(half):
        load_own(v).start()
        load_own(half + v).start()
        if v == 0:
            load_state.start()
            load_wind.start()
    load_offsets.start()
    load_coupling.start()
    load_var.start()

    def neighbour(side):
        return lax.rem(s + n_space - 1 + 2 * side, n_space)

    def send(src, dst, send_sem, recv_sem, where):
        return pltpu.make_async_remote_copy(
            src_ref=src,
            dst_ref=dst,
            send_sem=send_sem,
            recv_sem=recv_sem,
            device_id=where,
            device_id_type=MESH,
        )

    def mem_copy(h, k):
        v, level = k // per_var, lax.rem(k, per_var) * LEVELS_PER_CHUNK
        levels = pl.ds(level, LEVELS_PER_CHUNK)
        rows = pl.ds(pl.multiple_of((1 - h) * RADIUS, RADIUS), RADIUS)
        return send(
            own.at[:, half * h + v, levels, rows],
            halo.at[h, :, v, levels],
            mem_send.at[h, k],
            mem_recv.at[h, k],
            (t, neighbour(1 - h)),
        )

    def lam_copy(h):
        return send(
            lam_edge.at[h],
            lam_halo.at[h],
            lam_send.at[h],
            lam_recv.at[h],
            (t, neighbour(1 - h)),
        )

    def back_copy(h, k):
        v, level = k // per_var, lax.rem(k, per_var) * LEVELS_PER_CHUNK
        levels = pl.ds(level, LEVELS_PER_CHUNK)
        return send(
            back_out.at[h, v, levels],
            back_in.at[h, v, levels],
            back_send.at[h, k],
            back_recv.at[h, k],
            (t, neighbour(h)),
        )

    def part_of(ref, p):
        return ref.at[:, pl.ds(half_lev * p, half_lev)]

    def state_copy(p):
        return send(
            part_of(state_hbm.at[0], p),
            part_of(prev, p).at[:, :, pl.ds(8, width)],
            state_send.at[p],
            state_recv.at[p],
            (t_next, s),
        )

    def relay_in(slot):
        return send(
            part_of(state_hbm.at[0], min(slot, 1)),
            relayed.at[slot],
            relay_send.at[slot],
            relay_recv.at[slot],
            (t_next, relay_of),
        )

    def relay_out(slot):
        return send(
            relayed.at[slot],
            part_of(prev, min(slot, 1)).at[:, :, pl.ds(8, width)],
            relay_send.at[3 + slot],
            state_recv.at[min(slot, 1)],
            (t, served if slot < 2 else served_late),
        )

    last = chunks - 1
    last_levels = pl.ds(n_lev - LEVELS_PER_CHUNK, LEVELS_PER_CHUNK)
    facing = pl.ds(pl.multiple_of(parity * RADIUS, RADIUS), RADIUS)
    extra_copy = send(
        own.at[:, half * parity + half - 1, last_levels, facing],
        extra,
        extra_send.at[0],
        extra_recv.at[0],
        (t, neighbour(parity)),
    )
    extra_lam_copy = send(
        extra_lam_edge,
        extra_lam,
        extra_send.at[1],
        extra_recv.at[1],
        (t, neighbour(parity)),
    )

    def edge_copy(h):
        return send(
            state_edge.at[h],
            state_halo.at[h],
            edge_send.at[h],
            edge_recv.at[h],
            (t_next, neighbour(1 - h)),
        )

    def wind_copy(h):
        return send(
            wind_edge.at[h],
            wind_halo.at[h],
            wind_send.at[h],
            wind_recv.at[h],
            (t, neighbour(1 - h)),
        )

    pl.semaphore_wait(barrier, jnp.where(is_relay, 7, jnp.where(late, 6, 5)))
    load_lam.wait()
    for h in range(2):
        edge = lam[half * h : half * (h + 1), :, (1 - h) * RADIUS : (2 - h) * RADIUS]
        lam_edge[h] = edge.astype(jnp.bfloat16)
    extra_lam_edge[...] = lam[half * parity + half - 1, last_levels, facing].astype(jnp.bfloat16)
    load_own(0).wait()
    load_own(half).wait()
    for h in range(2):
        mem_copy(h, 0).start()
        lam_copy(h).start()

    @pl.when(~outer)
    def _():
        state_copy(0).start()
        state_copy(1).start()

    def start_members(k, carry):
        for h in range(2):
            mem_copy(h, k).start()
        return carry

    @pl.when(wrap)
    def _():
        relay_in(0).start()
        relay_in(1).start()
        extra_lam_copy.start()

    lax.fori_loop(1, per_var, start_members, 0)

    @pl.when(late)
    def _():
        relay_in(2).start()

    load_state.wait()
    load_wind.wait()
    for c in range(2):
        state_edge[0, c] = state[:, :, width - 2 + c]
        state_edge[1, c] = state[:, :, c]
    wind_edge[0] = wind[:, :, 8 + width - 1]
    wind_edge[1] = wind[:, :, 8]

    for h in range(2):
        edge_copy(h).start()
        wind_copy(h).start()
    for v in range(1, half):
        load_own(v).wait()
        load_own(half + v).wait()
        lax.fori_loop(per_var * v, per_var * (v + 1), start_members, 0)

    @pl.when(wrap)
    def _():
        extra_copy.start()

    size = GROUP * (width + RADIUS)
    block = 48

    def build(step, carry):
        side = step // (size // block)
        row_start = pl.multiple_of(lax.rem(step, size // block) * block, block)
        matrix = stencil_matrix(offsets, side, width, block, row_start)
        high = matrix.astype(jnp.bfloat16)
        rows = pl.ds(row_start, block)
        stencil[side, rows, :DEPTH] = high
        stencil[side, rows, DEPTH:] = (matrix - high.astype(jnp.float32)).astype(jnp.bfloat16)
        return carry

    load_offsets.wait()
    lax.fori_loop(0, 2 * (size // block), build, 0)
    def sums(side, full_v, level, lam_far, far_fields, near_products):
        lam_own = lam[full_v, level]
        own_sum = jnp.zeros((width, 128), jnp.float32)
        far_sum = jnp.zeros((RADIUS, 128), jnp.float32)
        for pair in range(members // (2 * GROUP)):
            fields, products = [], []
            for q in (2 * pair, 2 * pair + 1):
                near = own[pl.ds(q * GROUP, GROUP), full_v, level].astype(jnp.float32)
                far = far_fields(pl.ds(q * GROUP, GROUP)).astype(jnp.float32)
                fields.append((near, far))
                near = near * lam_own[None] if near_products else jnp.zeros_like(near)
                near = near.reshape(GROUP * width, 128)
                far = (far * lam_far[None]).reshape(GROUP * RADIUS, 128)
                rest = jnp.zeros((DEPTH - GROUP * (width + RADIUS), 128), jnp.float32)
                product = jnp.concatenate([near, far, rest], axis=0).astype(jnp.bfloat16)
                products.append(jnp.concatenate([product, product], axis=0))
            rhs = jnp.concatenate(products, axis=1)
            smooth = jnp.dot(stencil[side], rhs, preferred_element_type=jnp.float32)
            for i, (near, far) in enumerate(fields):
                part = smooth[:, 128 * i : 128 * (i + 1)]
                own_part = part[: GROUP * width].reshape(GROUP, width, 128)
                far_part = part[GROUP * width :].reshape(GROUP, RADIUS, 128)
                own_sum = own_sum + jnp.sum(near * own_part, axis=0)
                far_sum = far_sum + jnp.sum(far * far_part, axis=0)
        return own_sum, far_sum

    def one_level(side, v, level):
        own_sum, far_sum = sums(
            side,
            half * side + v,
            level,
            lam_halo[side, v, level].astype(jnp.float32),
            lambda group: halo[side, group, v, level],
            True,
        )
        total[half * side + v, level] = own_sum
        back_out[side, v, level] = far_sum.astype(jnp.bfloat16)

    def extra_level(d, carry):
        level = n_lev - LEVELS_PER_CHUNK + d
        own_sum, _ = sums(
            parity,
            half * (1 - parity) + half - 1,
            level,
            extra_lam[d].astype(jnp.float32),
            lambda group: extra[group, d],
            False,
        )
        near = jnp.where(parity == 0, own_sum[:RADIUS], own_sum[width - RADIUS :])
        total[half * (1 - parity) + half - 1, level, facing] += near
        back_in[1 - parity, half - 1, level] = jnp.zeros((RADIUS, 128), jnp.bfloat16)
        return carry

    def step(j, carry):
        turn = j - LEAD
        in_turn = (turn >= 0) & (j < 2 * chunks - LEAD)
        over_ici = jnp.where(in_turn, 1 - lax.rem(turn + 2 * chunks, 2), jnp.where(turn < 0, 0, 1))
        k = jnp.where(
            in_turn,
            jnp.where(over_ici == 1, turn // 2, LEAD + turn // 2),
            jnp.where(turn < 0, j, j - chunks),
        )
        side = lax.rem(parity + 1 - over_ici, 2)
        v, level = k // per_var, lax.rem(k, per_var) * LEVELS_PER_CHUNK

        @pl.when(k == 0)
        def _():
            lam_copy_wait(side)

        mem_copy(side, k).wait_recv()

        def each(d, c):
            one_level(side, v, level + d)
            return c

        lax.fori_loop(0, LEVELS_PER_CHUNK, each, 0, unroll=True)

        @pl.when(~(wrap & (side == parity) & (k == last)))
        def _():
            back_copy(side, k).start()

        for slot, at in ((0, chunks // 3), (1, chunks // 2), (2, (2 * chunks) // 3)):

            @pl.when(is_relay & (over_ici == 1) & (k == at))
            def _():
                relay_in(slot).wait_recv()
                relay_out(slot).start()

        @pl.when(late & (over_ici == 1) & (k == (2 * chunks) // 3))
        def _():
            state_copy(0).start()

        return carry

    def lam_copy_wait(h):
        send(
            lam_edge.at[h],
            lam_halo.at[h],
            lam_send.at[h],
            lam_recv.at[h],
            (t, neighbour(1 - h)),
        ).wait_recv()

    lax.fori_loop(0, 2 * chunks, step, 0)

    def drain_sends(k, carry):
        for h in range(2):
            mem_copy(h, k).wait_send()
        return carry

    def drain_back(k, carry):
        for h in range(2):

            @pl.when(~(wrap & (h == 1 - parity) & (k == last)))
            def _():
                back_copy(h, k).wait_recv()

        return carry

    def drain_back_sends(k, carry):
        for h in range(2):

            @pl.when(~(wrap & (h == parity) & (k == last)))
            def _():
                back_copy(h, k).wait_send()

        return carry

    lax.fori_loop(0, chunks, drain_sends, 0)
    load_coupling.wait()

    @pl.when(~wrap)
    def _():
        state_copy(0).wait_send()

    @pl.when(~outer)
    def _():
        state_copy(1).wait_send()

    @pl.when(wrap)
    def _():
        relay_in(0).wait_send()
        relay_in(1).wait_send()
        extra_copy.wait_send()
        extra_lam_copy.wait_send()

    @pl.when(late)
    def _():
        relay_in(2).wait_send()

    @pl.when(is_relay)
    def _():
        for slot in range(3):
            relay_out(slot).wait_send()

    for h in range(2):
        lam_copy(h).wait_send()
        edge_copy(h).wait_send()
        wind_copy(h).wait_send()

    for h in range(2):
        edge_copy(h).wait_recv()
        wind_copy(h).wait_recv()
    load_var.wait()
    padded = width + 16
    rows = lax.broadcasted_iota(jnp.int32, (padded, 128), 0)
    lanes = lax.broadcasted_iota(jnp.int32, (padded, 128), 1)
    wind[:, :, 7] = wind_halo[0]
    wind[:, :, 8 + width] = wind_halo[1]
    first = jnp.where(t == 0, 0.0, 1.0)

    def tangent(level, carry):
        inside = (rows >= 6) & (rows < 8 + width + 2)
        fields = [jnp.where(inside, prev[v, level], 0.0) for v in range(n_var)]
        wind_x = jnp.where(inside, wind[0, level], 0.0)
        wind_y = jnp.where(inside, wind[1, level], 0.0)
        x_up, x_down = jnp.maximum(wind_x, 0.0), jnp.minimum(wind_x, 0.0)
        y_up, y_down = jnp.maximum(wind_y, 0.0), jnp.minimum(wind_y, 0.0)
        for _ in range(2):
            new = []
            for v in range(n_var):
                f = fields[v]
                west = pltpu.roll(f, 1, 0)
                east = pltpu.roll(f, padded - 1, 0)
                south = jnp.where(lanes == 0, 0.0, pltpu.roll(f, 1, 1))
                north = jnp.where(lanes == 127, 0.0, pltpu.roll(f, 127, 1))
                moved = x_up * (f - west) + x_down * (east - f)
                moved = moved + y_up * (f - south) + y_down * (north - f)
                mixed = coupling[v, level, 0] * fields[0]
                for w in range(1, n_var):
                    mixed = mixed + coupling[v, level, w] * fields[w]
                new.append(f - moved + mixed)
            fields = new
        for v in range(n_var):
            propagated = jnp.where(first > 0.5, fields[v][8 : 8 + width], 0.0)
            base[v, level] = (
                0.5 * var[v, level] * lam[v, level] + state[v, level] - propagated
            )
        return carry

    for p in (1, 0):
        state_copy(p).wait_recv()
        levels = pl.ds(half_lev * p, half_lev)
        for c in range(2):
            prev[:, levels, 6 + c] = state_halo[0, c, :, levels]
            prev[:, levels, 8 + width + c] = state_halo[1, c, :, levels]
        lax.fori_loop(half_lev * p, half_lev * (p + 1), tangent, 0)

    @pl.when(wrap)
    def _():
        extra_copy.wait_recv()
        extra_lam_copy.wait_recv()
        lax.fori_loop(0, LEVELS_PER_CHUNK, extra_level, 0)


    scale = 0.5 / (members - 1)

    def compose(v, carry):
        out[0, v] = base[v] + scale * total[v]
        return carry

    lax.fori_loop(0, n_var, compose, 0)
    lax.fori_loop(0, chunks, drain_back_sends, 0)
    lax.fori_loop(0, chunks, drain_back, 0)
    for h in range(2):
        edge = pl.ds(0, RADIUS) if h == 1 else pl.ds(width - RADIUS, RADIUS)
        for v in range(half):
            out[0, half * h + v, :, edge] += scale * back_in[h, v].astype(jnp.float32)


def per_device(sizes, state, multiplier, members, static_var, courant, coupling, loc_offsets):
    _, n_mem, n_var, n_lev, width, lanes = members.shape
    half = n_var // 2
    chunks = half * (n_lev // LEVELS_PER_CHUNK)
    size = GROUP * (width + RADIUS)
    f32, bf16 = jnp.float32, jnp.bfloat16
    dma = pltpu.SemaphoreType.DMA
    hbm = pl.BlockSpec(memory_space=pltpu.HBM)
    offsets_shape = loc_offsets.shape
    coupling_shape = (n_var, n_lev, n_var)
    return pl.pallas_call(
        functools.partial(kernel, sizes),
        out_shape=jax.ShapeDtypeStruct(state.shape, f32),
        in_specs=[hbm] * 7,
        out_specs=pl.BlockSpec(memory_space=pltpu.VMEM),
        scratch_shapes=[
            pltpu.VMEM((n_mem, n_var, n_lev, width, lanes), bf16),
            pltpu.VMEM((2, n_mem, half, n_lev, RADIUS, lanes), bf16),
            pltpu.VMEM((n_var, n_lev, width, lanes), f32),
            pltpu.VMEM((2, half, n_lev, RADIUS, lanes), bf16),
            pltpu.VMEM((n_var, n_lev, width, lanes), f32),
            pltpu.VMEM((n_var, n_lev, width + 16, lanes), f32),
            pltpu.VMEM((n_var, n_lev, width, lanes), f32),
            pltpu.VMEM((2, n_lev, width + 16, lanes), f32),
            pltpu.VMEM((2, 2, n_var, n_lev, lanes), f32),
            pltpu.VMEM((2, 2, n_var, n_lev, lanes), f32),
            pltpu.VMEM((2, 2, n_lev, lanes), f32),
            pltpu.VMEM((2, 2, n_lev, lanes), f32),
            pltpu.VMEM((n_var, n_lev, width, lanes), f32),
            pltpu.VMEM((n_var, n_lev, width, lanes), f32),
            pltpu.VMEM((2, half, n_lev, RADIUS, lanes), bf16),
            pltpu.VMEM((2, half, n_lev, RADIUS, lanes), bf16),
            pltpu.VMEM((2, size, 2 * DEPTH), bf16),
            pltpu.VMEM((2, half, n_lev, RADIUS, lanes), bf16),
            pltpu.VMEM((LEVELS_PER_CHUNK, RADIUS, lanes), bf16),
            pltpu.VMEM((3, n_var, n_lev // 2, width, lanes), f32),
            pltpu.VMEM((n_mem, LEVELS_PER_CHUNK, RADIUS, lanes), bf16),
            pltpu.VMEM((LEVELS_PER_CHUNK, RADIUS, lanes), bf16),
            pltpu.SMEM(offsets_shape, jnp.int32),
            pltpu.SMEM(coupling_shape, f32),
            dma((6,)),
            dma((n_var,)),
            dma((2, chunks)),
            dma((2, chunks)),
            dma((2, chunks)),
            dma((2, chunks)),
            dma((2,)),
            dma((2,)),
            dma((2,)),
            dma((2,)),
            dma((2,)),
            dma((2,)),
            dma((2,)),
            dma((2,)),
            dma((6,)),
            dma((3,)),
            dma((2,)),
            dma((2,)),
        ],
        compiler_params=pltpu.CompilerParams(
            collective_id=0, has_side_effects=True, vmem_limit_bytes=48 * 1024 * 1024
        ),
        name="hybrid_row",
    )(*[pltpu.with_memory_space_constraint(x, pltpu.HBM) for x in (loc_offsets, jnp.transpose(coupling, (1, 0, 2)), state, multiplier, members, static_var, courant)])


def solution(mesh):
    sizes = (mesh.shape["tm"], mesh.shape["space"])
    return jax.shard_map(
        functools.partial(per_device, sizes),
        mesh=mesh,
        in_specs=(
            P("tm", None, None, "space", None),
            P("tm", None, None, "space", None),
            P("tm", None, None, None, "space", None),
            P("tm", None, None, "space", None),
            P("tm", None, None, "space", None),
            P(),
            P(),
        ),
        out_specs=P("tm", None, None, "space", None),
        check_vma=False,
    )
```

```python
import functools
import jax
import jax.numpy as jnp
from jax import lax
from jax.experimental import pallas as pl
from jax.experimental.pallas import tpu as pltpu
from jax.sharding import PartitionSpec as P

MESH = pl.DeviceIdType.MESH
GROUP = 10
DEPTH = 256
LEAD = 4
RADIUS = 8
LEVELS_PER_CHUNK = 2


def column_of(index, width, side):
    own = GROUP * width
    in_halo = index >= own
    halo_index = index - own
    member = jnp.where(in_halo, halo_index >> 3, index >> 4)
    halo_column = (halo_index & 7) + jnp.where(side == 0, -RADIUS, width)
    column = jnp.where(in_halo, halo_column, index & (width - 1))
    return member, column, in_halo


def stencil_matrix(offsets, side, width, rows, row_start):
    shape = (rows, DEPTH)
    row = lax.broadcasted_iota(jnp.int32, shape, 0) + row_start
    col = lax.broadcasted_iota(jnp.int32, shape, 1)
    row_member, row_column, row_halo = column_of(row, width, side)
    col_member, col_column, col_halo = column_of(col, width, side)
    distance = col_column - row_column
    count = jnp.zeros(shape, jnp.float32)
    for j in range(offsets.shape[0]):
        count = count + jnp.where(distance == offsets[j], 1.0, 0.0)
    keep = (row_member == col_member) & ~(row_halo & col_halo)
    scaled = distance.astype(jnp.float32) * (1.0 / RADIUS)
    return jnp.where(keep, count * jnp.exp(-0.5 * scaled * scaled), 0.0)


def kernel(
    sizes,
    offsets_hbm,
    coupling_hbm,
    state_hbm,
    mult_hbm,
    mem_hbm,
    var_hbm,
    wind_hbm,
    out,
    own,
    halo,
    lam,
    lam_halo,
    state,
    prev,
    var,
    wind,
    state_edge,
    state_halo,
    wind_edge,
    wind_halo,
    total,
    base,
    back_out,
    back_in,
    stencil,
    lam_edge,
    extra_lam_edge,
    relayed,
    extra,
    extra_lam,
    offsets,
    coupling,
    local_sem,
    own_sem,
    mem_send,
    mem_recv,
    back_send,
    back_recv,
    lam_send,
    lam_recv,
    state_send,
    state_recv,
    edge_send,
    edge_recv,
    wind_send,
    wind_recv,
    relay_send,
    relay_recv,
    extra_send,
    extra_recv,
):
    n_tm, n_space = sizes
    members, n_var, n_lev, width, _ = own.shape
    half, half_lev = n_var // 2, n_lev // 2
    per_var = n_lev // LEVELS_PER_CHUNK
    chunks = half * per_var
    t = lax.axis_index("tm")
    s = lax.axis_index("space")
    parity = lax.rem(s, 2)
    t_next, t_last = lax.rem(t + 1, n_tm), lax.rem(t + n_tm - 1, n_tm)
    s_next, s_last = lax.rem(s + 1, n_space), lax.rem(s + n_space - 1, n_space)

    planes = n_space // 4
    run = (s // (2 * planes)) * (2 * planes)
    z = lax.rem(s // 2, planes)
    outer = (z == 0) | (z == planes - 1)
    relay_of = jnp.where(z == 0, run + 3, run + 2 * (planes - 2))
    wrap = ((z == 0) & (parity == 0)) | ((z == planes - 1) & (parity == 1))
    late = outer & ~wrap
    is_relay = (s == run + 3) | (s == run + 2 * (planes - 2))
    served = jnp.where(z == 1, run, run + 2 * planes - 1)
    served_late = jnp.where(z == 1, run + 1, run + 2 * planes - 2)

    barrier = pltpu.get_barrier_semaphore()

    def greet(*peer):
        pl.semaphore_signal(barrier, inc=1, device_id=peer, device_id_type=MESH)

    greet(t, s_next)
    greet(t, s_last)
    greet(t_last, s_next)
    greet(t_last, s_last)
    greet(jnp.where(wrap, t, t_last), jnp.where(wrap, relay_of, s))

    @pl.when(late)
    def _():
        greet(t, relay_of)

    @pl.when(is_relay)
    def _():
        greet(t_last, served)
        greet(t_last, served_late)

    load_state = pltpu.make_async_copy(state_hbm.at[0], state, local_sem.at[0])
    load_wind = pltpu.make_async_copy(
        wind_hbm.at[0], wind.at[:, :, pl.ds(8, width)], local_sem.at[1]
    )
    load_lam = pltpu.make_async_copy(mult_hbm.at[0], lam, local_sem.at[2])
    load_var = pltpu.make_async_copy(var_hbm.at[0], var, local_sem.at[3])
    def load_own(v):
        return pltpu.make_async_copy(mem_hbm.at[0, :, v], own.at[:, v], own_sem.at[v])

    load_offsets = pltpu.make_async_copy(offsets_hbm, offsets, local_sem.at[4])
    load_coupling = pltpu.make_async_copy(coupling_hbm, coupling, local_sem.at[5])
    load_lam.start()
    for v in range(half):
        load_own(v).start()
        load_own(half + v).start()
        if v == 0:
            load_state.start()
            load_wind.start()
    load_offsets.start()
    load_coupling.start()
    load_var.start()

    def neighbour(side):
        return lax.rem(s + n_space - 1 + 2 * side, n_space)

    def send(src, dst, send_sem, recv_sem, where):
        return pltpu.make_async_remote_copy(
            src_ref=src,
            dst_ref=dst,
            send_sem=send_sem,
            recv_sem=recv_sem,
            device_id=where,
            device_id_type=MESH,
        )

    def mem_copy(h, k):
        v, level = k // per_var, lax.rem(k, per_var) * LEVELS_PER_CHUNK
        levels = pl.ds(level, LEVELS_PER_CHUNK)
        rows = pl.ds(pl.multiple_of((1 - h) * RADIUS, RADIUS), RADIUS)
        return send(
            own.at[:, half * h + v, levels, rows],
            halo.at[h, :, v, levels],
            mem_send.at[h, k],
            mem_recv.at[h, k],
            (t, neighbour(1 - h)),
        )

    def lam_copy(h):
        return send(
            lam_edge.at[h],
            lam_halo.at[h],
            lam_send.at[h],
            lam_recv.at[h],
            (t, neighbour(1 - h)),
        )

    def back_copy(h, k):
        v, level = k // per_var, lax.rem(k, per_var) * LEVELS_PER_CHUNK
        levels = pl.ds(level, LEVELS_PER_CHUNK)
        return send(
            back_out.at[h, v, levels],
            back_in.at[h, v, levels],
            back_send.at[h, k],
            back_recv.at[h, k],
            (t, neighbour(h)),
        )

    def part_of(ref, p):
        return ref.at[:, pl.ds(half_lev * p, half_lev)]

    def state_copy(p):
        return send(
            part_of(state_hbm.at[0], p),
            part_of(prev, p).at[:, :, pl.ds(8, width)],
            state_send.at[p],
            state_recv.at[p],
            (t_next, s),
        )

    def relay_in(slot):
        return send(
            part_of(state_hbm.at[0], min(slot, 1)),
            relayed.at[slot],
            relay_send.at[slot],
            relay_recv.at[slot],
            (t_next, relay_of),
        )

    def relay_out(slot):
        return send(
            relayed.at[slot],
            part_of(prev, min(slot, 1)).at[:, :, pl.ds(8, width)],
            relay_send.at[3 + slot],
            state_recv.at[min(slot, 1)],
            (t, served if slot < 2 else served_late),
        )

    last = chunks - 1
    last_levels = pl.ds(n_lev - LEVELS_PER_CHUNK, LEVELS_PER_CHUNK)
    facing = pl.ds(pl.multiple_of(parity * RADIUS, RADIUS), RADIUS)
    extra_copy = send(
        own.at[:, half * parity + half - 1, last_levels, facing],
        extra,
        extra_send.at[0],
        extra_recv.at[0],
        (t, neighbour(parity)),
    )
    extra_lam_copy = send(
        extra_lam_edge,
        extra_lam,
        extra_send.at[1],
        extra_recv.at[1],
        (t, neighbour(parity)),
    )

    def edge_copy(h):
        return send(
            state_edge.at[h],
            state_halo.at[h],
            edge_send.at[h],
            edge_recv.at[h],
            (t_next, neighbour(1 - h)),
        )

    def wind_copy(h):
        return send(
            wind_edge.at[h],
            wind_halo.at[h],
            wind_send.at[h],
            wind_recv.at[h],
            (t, neighbour(1 - h)),
        )

    pl.semaphore_wait(barrier, jnp.where(is_relay, 7, jnp.where(late, 6, 5)))
    load_lam.wait()
    for h in range(2):
        edge = lam[half * h : half * (h + 1), :, (1 - h) * RADIUS : (2 - h) * RADIUS]
        lam_edge[h] = edge.astype(jnp.bfloat16)
    extra_lam_edge[...] = lam[half * parity + half - 1, last_levels, facing].astype(jnp.bfloat16)
    load_own(0).wait()
    load_own(half).wait()
    for h in range(2):
        mem_copy(h, 0).start()
        lam_copy(h).start()

    @pl.when(~outer)
    def _():
        state_copy(0).start()
        state_copy(1).start()

    def start_members(k, carry):
        for h in range(2):
            mem_copy(h, k).start()
        return carry

    @pl.when(wrap)
    def _():
        relay_in(0).start()
        relay_in(1).start()
        extra_lam_copy.start()

    lax.fori_loop(1, per_var, start_members, 0)

    @pl.when(late)
    def _():
        relay_in(2).start()

    load_state.wait()
    load_wind.wait()
    for c in range(2):
        state_edge[0, c] = state[:, :, width - 2 + c]
        state_edge[1, c] = state[:, :, c]
    wind_edge[0] = wind[:, :, 8 + width - 1]
    wind_edge[1] = wind[:, :, 8]

    def start_edges():
        for h in range(2):
            edge_copy(h).start()
            wind_copy(h).start()

    pl.when(~wrap)(start_edges)
    for v in range(1, half):
        load_own(v).wait()
        load_own(half + v).wait()
        lax.fori_loop(per_var * v, min(per_var * (v + 1), last), start_members, 0)

    pl.when(wrap)(start_edges)
    start_members(last, 0)

    @pl.when(wrap)
    def _():
        extra_copy.start()

    size = GROUP * (width + RADIUS)
    block = 48

    def build(step, carry):
        side = step // (size // block)
        row_start = pl.multiple_of(lax.rem(step, size // block) * block, block)
        matrix = stencil_matrix(offsets, side, width, block, row_start)
        high = matrix.astype(jnp.bfloat16)
        rows = pl.ds(row_start, block)
        stencil[side, rows, :DEPTH] = high
        stencil[side, rows, DEPTH:] = (matrix - high.astype(jnp.float32)).astype(jnp.bfloat16)
        return carry

    load_offsets.wait()
    lax.fori_loop(0, 2 * (size // block), build, 0)
    def sums(side, full_v, level, lam_far, far_fields, near_products):
        lam_own = lam[full_v, level]
        own_sum = jnp.zeros((width, 128), jnp.float32)
        far_sum = jnp.zeros((RADIUS, 128), jnp.float32)
        for pair in range(members // (2 * GROUP)):
            fields, products = [], []
            for q in (2 * pair, 2 * pair + 1):
                near = own[pl.ds(q * GROUP, GROUP), full_v, level].astype(jnp.float32)
                far = far_fields(pl.ds(q * GROUP, GROUP)).astype(jnp.float32)
                fields.append((near, far))
                near = near * lam_own[None] if near_products else jnp.zeros_like(near)
                near = near.reshape(GROUP * width, 128)
                far = (far * lam_far[None]).reshape(GROUP * RADIUS, 128)
                rest = jnp.zeros((DEPTH - GROUP * (width + RADIUS), 128), jnp.float32)
                product = jnp.concatenate([near, far, rest], axis=0).astype(jnp.bfloat16)
                products.append(jnp.concatenate([product, product], axis=0))
            rhs = jnp.concatenate(products, axis=1)
            smooth = jnp.dot(stencil[side], rhs, preferred_element_type=jnp.float32)
            for i, (near, far) in enumerate(fields):
                part = smooth[:, 128 * i : 128 * (i + 1)]
                own_part = part[: GROUP * width].reshape(GROUP, width, 128)
                far_part = part[GROUP * width :].reshape(GROUP, RADIUS, 128)
                own_sum = own_sum + jnp.sum(near * own_part, axis=0)
                far_sum = far_sum + jnp.sum(far * far_part, axis=0)
        return own_sum, far_sum

    def one_level(side, v, level):
        own_sum, far_sum = sums(
            side,
            half * side + v,
            level,
            lam_halo[side, v, level].astype(jnp.float32),
            lambda group: halo[side, group, v, level],
            True,
        )
        total[half * side + v, level] = own_sum
        back_out[side, v, level] = far_sum.astype(jnp.bfloat16)

    def extra_level(d, carry):
        level = n_lev - LEVELS_PER_CHUNK + d
        own_sum, _ = sums(
            parity,
            half * (1 - parity) + half - 1,
            level,
            extra_lam[d].astype(jnp.float32),
            lambda group: extra[group, d],
            False,
        )
        near = jnp.where(parity == 0, own_sum[:RADIUS], own_sum[width - RADIUS :])
        total[half * (1 - parity) + half - 1, level, facing] += near
        back_in[1 - parity, half - 1, level] = jnp.zeros((RADIUS, 128), jnp.bfloat16)
        return carry

    def step(j, carry):
        turn = j - LEAD
        in_turn = (turn >= 0) & (j < 2 * chunks - LEAD)
        over_ici = jnp.where(in_turn, 1 - lax.rem(turn + 2 * chunks, 2), jnp.where(turn < 0, 0, 1))
        k = jnp.where(
            in_turn,
            jnp.where(over_ici == 1, turn // 2, LEAD + turn // 2),
            jnp.where(turn < 0, j, j - chunks),
        )
        side = lax.rem(parity + 1 - over_ici, 2)
        v, level = k // per_var, lax.rem(k, per_var) * LEVELS_PER_CHUNK

        @pl.when(k == 0)
        def _():
            lam_copy_wait(side)

        mem_copy(side, k).wait_recv()

        def each(d, c):
            one_level(side, v, level + d)
            return c

        lax.fori_loop(0, LEVELS_PER_CHUNK, each, 0, unroll=True)

        @pl.when(~(wrap & (side == parity) & (k == last)))
        def _():
            back_copy(side, k).start()

        for slot, at in ((0, chunks // 3), (1, chunks // 2), (2, (2 * chunks) // 3)):

            @pl.when(is_relay & (over_ici == 1) & (k == at))
            def _():
                relay_in(slot).wait_recv()
                relay_out(slot).start()

        @pl.when(late & (over_ici == 1) & (k == (2 * chunks) // 3))
        def _():
            state_copy(0).start()

        return carry

    def lam_copy_wait(h):
        send(
            lam_edge.at[h],
            lam_halo.at[h],
            lam_send.at[h],
            lam_recv.at[h],
            (t, neighbour(1 - h)),
        ).wait_recv()

    lax.fori_loop(0, 2 * chunks, step, 0)

    def drain_sends(k, carry):
        for h in range(2):
            mem_copy(h, k).wait_send()
        return carry

    def drain_back(k, carry):
        for h in range(2):

            @pl.when(~(wrap & (h == 1 - parity) & (k == last)))
            def _():
                back_copy(h, k).wait_recv()

        return carry

    def drain_back_sends(k, carry):
        for h in range(2):

            @pl.when(~(wrap & (h == parity) & (k == last)))
            def _():
                back_copy(h, k).wait_send()

        return carry

    lax.fori_loop(0, chunks, drain_sends, 0)
    load_coupling.wait()

    @pl.when(~wrap)
    def _():
        state_copy(0).wait_send()

    @pl.when(~outer)
    def _():
        state_copy(1).wait_send()

    @pl.when(wrap)
    def _():
        relay_in(0).wait_send()
        relay_in(1).wait_send()
        extra_copy.wait_send()
        extra_lam_copy.wait_send()

    @pl.when(late)
    def _():
        relay_in(2).wait_send()

    @pl.when(is_relay)
    def _():
        for slot in range(3):
            relay_out(slot).wait_send()

    for h in range(2):
        lam_copy(h).wait_send()
        edge_copy(h).wait_send()
        wind_copy(h).wait_send()

    for h in range(2):
        edge_copy(h).wait_recv()
        wind_copy(h).wait_recv()
    load_var.wait()
    padded = width + 16
    rows = lax.broadcasted_iota(jnp.int32, (padded, 128), 0)
    lanes = lax.broadcasted_iota(jnp.int32, (padded, 128), 1)
    wind[:, :, 7] = wind_halo[0]
    wind[:, :, 8 + width] = wind_halo[1]
    first = jnp.where(t == 0, 0.0, 1.0)

    def tangent(level, carry):
        inside = (rows >= 6) & (rows < 8 + width + 2)
        fields = [jnp.where(inside, prev[v, level], 0.0) for v in range(n_var)]
        wind_x = jnp.where(inside, wind[0, level], 0.0)
        wind_y = jnp.where(inside, wind[1, level], 0.0)
        x_up, x_down = jnp.maximum(wind_x, 0.0), jnp.minimum(wind_x, 0.0)
        y_up, y_down = jnp.maximum(wind_y, 0.0), jnp.minimum(wind_y, 0.0)
        for _ in range(2):
            new = []
            for v in range(n_var):
                f = fields[v]
                west = pltpu.roll(f, 1, 0)
                east = pltpu.roll(f, padded - 1, 0)
                south = jnp.where(lanes == 0, 0.0, pltpu.roll(f, 1, 1))
                north = jnp.where(lanes == 127, 0.0, pltpu.roll(f, 127, 1))
                moved = x_up * (f - west) + x_down * (east - f)
                moved = moved + y_up * (f - south) + y_down * (north - f)
                mixed = coupling[v, level, 0] * fields[0]
                for w in range(1, n_var):
                    mixed = mixed + coupling[v, level, w] * fields[w]
                new.append(f - moved + mixed)
            fields = new
        for v in range(n_var):
            propagated = jnp.where(first > 0.5, fields[v][8 : 8 + width], 0.0)
            base[v, level] = (
                0.5 * var[v, level] * lam[v, level] + state[v, level] - propagated
            )
        return carry

    for p in (1, 0):
        state_copy(p).wait_recv()
        levels = pl.ds(half_lev * p, half_lev)
        for c in range(2):
            prev[:, levels, 6 + c] = state_halo[0, c, :, levels]
            prev[:, levels, 8 + width + c] = state_halo[1, c, :, levels]
        lax.fori_loop(half_lev * p, half_lev * (p + 1), tangent, 0)

    @pl.when(wrap)
    def _():
        extra_copy.wait_recv()
        extra_lam_copy.wait_recv()
        lax.fori_loop(0, LEVELS_PER_CHUNK, extra_level, 0)


    scale = 0.5 / (members - 1)

    def compose(v, carry):
        out[0, v] = base[v] + scale * total[v]
        return carry

    lax.fori_loop(0, n_var, compose, 0)
    lax.fori_loop(0, chunks, drain_back_sends, 0)
    lax.fori_loop(0, chunks, drain_back, 0)
    for h in range(2):
        edge = pl.ds(0, RADIUS) if h == 1 else pl.ds(width - RADIUS, RADIUS)
        for v in range(half):
            out[0, half * h + v, :, edge] += scale * back_in[h, v].astype(jnp.float32)


def per_device(sizes, state, multiplier, members, static_var, courant, coupling, loc_offsets):
    _, n_mem, n_var, n_lev, width, lanes = members.shape
    half = n_var // 2
    chunks = half * (n_lev // LEVELS_PER_CHUNK)
    size = GROUP * (width + RADIUS)
    f32, bf16 = jnp.float32, jnp.bfloat16
    dma = pltpu.SemaphoreType.DMA
    hbm = pl.BlockSpec(memory_space=pltpu.HBM)
    offsets_shape = loc_offsets.shape
    coupling_shape = (n_var, n_lev, n_var)
    return pl.pallas_call(
        functools.partial(kernel, sizes),
        out_shape=jax.ShapeDtypeStruct(state.shape, f32),
        in_specs=[hbm] * 7,
        out_specs=pl.BlockSpec(memory_space=pltpu.VMEM),
        scratch_shapes=[
            pltpu.VMEM((n_mem, n_var, n_lev, width, lanes), bf16),
            pltpu.VMEM((2, n_mem, half, n_lev, RADIUS, lanes), bf16),
            pltpu.VMEM((n_var, n_lev, width, lanes), f32),
            pltpu.VMEM((2, half, n_lev, RADIUS, lanes), bf16),
            pltpu.VMEM((n_var, n_lev, width, lanes), f32),
            pltpu.VMEM((n_var, n_lev, width + 16, lanes), f32),
            pltpu.VMEM((n_var, n_lev, width, lanes), f32),
            pltpu.VMEM((2, n_lev, width + 16, lanes), f32),
            pltpu.VMEM((2, 2, n_var, n_lev, lanes), f32),
            pltpu.VMEM((2, 2, n_var, n_lev, lanes), f32),
            pltpu.VMEM((2, 2, n_lev, lanes), f32),
            pltpu.VMEM((2, 2, n_lev, lanes), f32),
            pltpu.VMEM((n_var, n_lev, width, lanes), f32),
            pltpu.VMEM((n_var, n_lev, width, lanes), f32),
            pltpu.VMEM((2, half, n_lev, RADIUS, lanes), bf16),
            pltpu.VMEM((2, half, n_lev, RADIUS, lanes), bf16),
            pltpu.VMEM((2, size, 2 * DEPTH), bf16),
            pltpu.VMEM((2, half, n_lev, RADIUS, lanes), bf16),
            pltpu.VMEM((LEVELS_PER_CHUNK, RADIUS, lanes), bf16),
            pltpu.VMEM((3, n_var, n_lev // 2, width, lanes), f32),
            pltpu.VMEM((n_mem, LEVELS_PER_CHUNK, RADIUS, lanes), bf16),
            pltpu.VMEM((LEVELS_PER_CHUNK, RADIUS, lanes), bf16),
            pltpu.SMEM(offsets_shape, jnp.int32),
            pltpu.SMEM(coupling_shape, f32),
            dma((6,)),
            dma((n_var,)),
            dma((2, chunks)),
            dma((2, chunks)),
            dma((2, chunks)),
            dma((2, chunks)),
            dma((2,)),
            dma((2,)),
            dma((2,)),
            dma((2,)),
            dma((2,)),
            dma((2,)),
            dma((2,)),
            dma((2,)),
            dma((6,)),
            dma((3,)),
            dma((2,)),
            dma((2,)),
        ],
        compiler_params=pltpu.CompilerParams(
            collective_id=0, has_side_effects=True, vmem_limit_bytes=48 * 1024 * 1024
        ),
        name="hybrid_row",
    )(*[pltpu.with_memory_space_constraint(x, pltpu.HBM) for x in (loc_offsets, jnp.transpose(coupling, (1, 0, 2)), state, multiplier, members, static_var, courant)])


def solution(mesh):
    sizes = (mesh.shape["tm"], mesh.shape["space"])
    return jax.shard_map(
        functools.partial(per_device, sizes),
        mesh=mesh,
        in_specs=(
            P("tm", None, None, "space", None),
            P("tm", None, None, "space", None),
            P("tm", None, None, None, "space", None),
            P("tm", None, None, "space", None),
            P("tm", None, None, "space", None),
            P(),
            P(),
        ),
        out_specs=P("tm", None, None, "space", None),
        check_vma=False,
    )
```
